128 devices in a mesh: stage: 2 (over core), data: 64 (over z, y, x).
Axes of the slice: x: 4, y: 4, z: 4, core: 2. Of those that a mesh axis runs over, the one named last changes fastest.
Arguments:
- x_in: bfloat16 [16, 2048, 768], P(None, 'data')
- targets: bfloat16 [16, 2048, 768], P(None, 'data')
- w1_bf: bfloat16 [2, 2, 1, 768, 3072], P('stage')
- w2_bf: bfloat16 [2, 2, 1, 3072, 768], P('stage')
- w_master: float32 [2, 2, 1, 4718592], P('stage', None, None, 'data')
- m_state: float32 [2, 2, 1, 4718592], P('stage', None, None, 'data')
- v_state: float32 [2, 2, 1, 4718592], P('stage', None, None, 'data')
Outputs:
- output 1: bfloat16 [2, 2, 1, 768, 3072], P('stage')
- output 2: bfloat16 [2, 2, 1, 3072, 768], P('stage')
- output 3: float32 [2, 2, 1, 4718592], P('stage', None, None, 'data')
- output 4: float32 [2, 2, 1, 4718592], P('stage', None, None, 'data')
- output 5: float32 [2, 2, 1, 4718592], P('stage', None, None, 'data')
- output 6: float32 [], replicated
All inputs are finite; a program needn't handle non-finite values.
Results may differ from the reference program's by a relative error of at most 0.001.
Values are sent between devices in bfloat16 or wider.
A program may use at most 1 GiB of HBM per device.

```python
import math
import jax
import jax.numpy as jnp
from jax import lax

STAGES = 2
DATA_WAYS = 64
MB_GROUPS = 8
TOK_DEV = 32
VSTAGE_BLOCKS = 1
D_MODEL = 768
ADAM_STEP = 1000

N_MICRO = MB_GROUPS * STAGES
N_ROWS = DATA_WAYS * TOK_DEV
D_FF = 4 * D_MODEL
N_BLOCKS = 2 * STAGES * VSTAGE_BLOCKS
N_TOKENS = N_MICRO * N_ROWS
FLAT_LEN = 8 * D_MODEL * D_MODEL
N_PARAMS = N_BLOCKS * FLAT_LEN
BETA_ONE = 0.9
BETA_TWO = 0.999
ADAM_EPS = 1e-8
WEIGHT_DECAY = 0.1
TAU_CLIP = 0.3 * D_MODEL * math.sqrt(N_BLOCKS * (3.0 / N_TOKENS + 0.008))
LEARN_RATE = 0.1 / math.sqrt(4.0 * D_MODEL * N_BLOCKS)


def gelu_tanh(pre_act):
    return jax.nn.gelu(pre_act, approximate=True)


def moment_scale():
    scale_two = TAU_CLIP * math.sqrt(2.0 / (N_PARAMS * (1.0 + 1.0 / N_BLOCKS)))
    scale_one = scale_two / math.sqrt(N_BLOCKS)
    return jnp.concatenate([jnp.full((D_MODEL * D_FF,), scale_one, jnp.float32), jnp.full((D_FF * D_MODEL,), scale_two, jnp.float32)])


def setup_inputs(seed: int = 0) -> dict:
    key_list = jax.random.split(jax.random.key(seed), 6)
    act_shape = (N_MICRO, N_ROWS, D_MODEL)
    lead_dims = (STAGES, 2, VSTAGE_BLOCKS)
    x_in = jax.random.normal(key_list[0], act_shape, jnp.float32)
    targets = jax.random.normal(key_list[1], act_shape, jnp.float32)
    w_one = jax.random.normal(key_list[2], lead_dims + (D_MODEL, D_FF), jnp.float32) * D_MODEL ** -0.5
    w_two = jax.random.normal(key_list[3], lead_dims + (D_FF, D_MODEL), jnp.float32) * (D_FF * N_BLOCKS) ** -0.5
    w_master = jnp.concatenate([w_one.reshape(lead_dims + (-1,)), w_two.reshape(lead_dims + (-1,))], axis=-1)
    elem_scale = moment_scale()
    m_state = 0.5 * elem_scale * jax.random.normal(key_list[4], w_master.shape, jnp.float32)
    v_state = elem_scale * elem_scale * (0.25 + 0.5 * jax.random.uniform(key_list[5], w_master.shape, jnp.float32))
    return dict(x_in=x_in.astype(jnp.bfloat16), targets=targets.astype(jnp.bfloat16), w1_bf=w_one.astype(jnp.bfloat16), w2_bf=w_two.astype(jnp.bfloat16), w_master=w_master, m_state=m_state, v_state=v_state)


def block_forward(h_in, w_one, w_two):
    pre_act = jnp.dot(h_in, w_one, preferred_element_type=jnp.float32)
    act_bf = gelu_tanh(pre_act).astype(jnp.bfloat16)
    out_val = h_in.astype(jnp.float32) + jnp.dot(act_bf, w_two, preferred_element_type=jnp.float32)
    return out_val.astype(jnp.bfloat16)


def block_backward(h_in, grad_out, w_one, w_two):
    pre_act = jnp.dot(h_in, w_one, preferred_element_type=jnp.float32)
    act_val, gelu_pull = jax.vjp(gelu_tanh, pre_act)
    act_bf = act_val.astype(jnp.bfloat16)
    grad_act = jnp.dot(grad_out, w_two.T, preferred_element_type=jnp.float32)
    grad_pre = gelu_pull(grad_act)[0].astype(jnp.bfloat16)
    back_val = jnp.dot(grad_pre, w_one.T, preferred_element_type=jnp.float32)
    grad_in = (grad_out.astype(jnp.float32) + back_val).astype(jnp.bfloat16)
    grad_one = jnp.dot(h_in.T, grad_pre, preferred_element_type=jnp.float32)
    grad_two = jnp.dot(act_bf.T, grad_out, preferred_element_type=jnp.float32)
    return grad_in, grad_one, grad_two


def reference(x_in, targets, w1_bf, w2_bf, w_master, m_state, v_state):
    w_ones = jnp.swapaxes(w1_bf, 0, 1).reshape(N_BLOCKS, D_MODEL, D_FF)
    w_twos = jnp.swapaxes(w2_bf, 0, 1).reshape(N_BLOCKS, D_FF, D_MODEL)

    def fwd_step(h_in, weights):
        return block_forward(h_in, weights[0], weights[1]), h_in

    def bwd_step(grad_out, saved_item):
        grad_in, grad_one, grad_two = block_backward(saved_item[0], grad_out, saved_item[1], saved_item[2])
        return grad_in, (grad_one, grad_two)

    def micro_step(state_carry, mb_pair):
        acc_one, acc_two, loss_acc = state_carry
        h_out, block_inputs = lax.scan(fwd_step, mb_pair[0], (w_ones, w_twos))
        residual = h_out.astype(jnp.float32) - mb_pair[1].astype(jnp.float32)
        loss_acc = loss_acc + 0.5 * jnp.sum(residual * residual)
        grad_seed = (residual / N_TOKENS).astype(jnp.bfloat16)
        grad_pair = lax.scan(bwd_step, grad_seed, (block_inputs, w_ones, w_twos), reverse=True)[1]
        return (acc_one + grad_pair[0], acc_two + grad_pair[1], loss_acc), None

    start_carry = (jnp.zeros((N_BLOCKS, D_MODEL, D_FF), jnp.float32), jnp.zeros((N_BLOCKS, D_FF, D_MODEL), jnp.float32), jnp.zeros((), jnp.float32))
    acc_one, acc_two, loss_acc = lax.scan(micro_step, start_carry, (x_in, targets))[0]
    flat_dims = (2, STAGES, VSTAGE_BLOCKS, -1)
    grad_flat = jnp.swapaxes(jnp.concatenate([acc_one.reshape(flat_dims), acc_two.reshape(flat_dims)], axis=-1), 0, 1)
    grad_norm = jnp.sqrt(jnp.sum(grad_flat * grad_flat))
    clip_factor = jnp.minimum(1.0, TAU_CLIP / grad_norm)
    grad_clip = clip_factor * grad_flat
    m_new = BETA_ONE * m_state + (1.0 - BETA_ONE) * grad_clip
    v_new = BETA_TWO * v_state + (1.0 - BETA_TWO) * grad_clip * grad_clip
    m_hat = m_new / (1.0 - BETA_ONE ** ADAM_STEP)
    v_hat = v_new / (1.0 - BETA_TWO ** ADAM_STEP)
    w_new = w_master - LEARN_RATE * (m_hat / (jnp.sqrt(v_hat) + ADAM_EPS) + WEIGHT_DECAY * w_master)
    w_bf = w_new.astype(jnp.bfloat16)
    split_at = D_MODEL * D_FF
    w1_new = w_bf[..., :split_at].reshape(STAGES, 2, VSTAGE_BLOCKS, D_MODEL, D_FF)
    w2_new = w_bf[..., split_at:].reshape(STAGES, 2, VSTAGE_BLOCKS, D_FF, D_MODEL)
    return w1_new, w2_new, w_new, m_new, v_new, loss_acc / N_TOKENS
```

```python
import math
import jax
import jax.numpy as jnp
from jax import lax
from jax.sharding import PartitionSpec as P

BETA_ONE = 0.9
BETA_TWO = 0.999
ADAM_EPS = 1e-8
WEIGHT_DECAY = 0.1
ADAM_STEP = 1000


def gelu_tanh(pre_act):
    return jax.nn.gelu(pre_act, approximate=True)


def dot32(lhs, rhs, dims):
    return lax.dot_general(lhs, rhs, (dims, ((), ())), preferred_element_type=jnp.float32)


def to_tiles(mat):
    rows, cols = mat.shape
    return mat.reshape(rows // 8, 8, cols // 128, 128).transpose(0, 2, 1, 3).reshape(-1, 8, 128)


def from_tiles(tiles, rows, cols):
    return tiles.reshape(rows // 8, cols // 128, 8, 128).transpose(0, 2, 1, 3).reshape(rows, cols)


def run_stack(x_all, t_all, w1_loc, w2_loc, n_tokens, n_chunk):
    stage_idx = lax.axis_index("stage")
    on_first = stage_idx == 0
    n_rows, d_model = x_all.shape
    n_tok = n_rows // n_chunk
    n_items = 2 * n_chunk
    n_ticks = n_items + 1
    swap = [(0, 1), (1, 0)]

    def weights(half_first, half_second):
        if half_first == half_second:
            return w1_loc[half_first], w2_loc[half_first]
        return (jnp.where(on_first, w1_loc[half_first], w1_loc[half_second]),
                jnp.where(on_first, w2_loc[half_first], w2_loc[half_second]))

    def half_of(item, backward):
        half = min(max(item, 0), n_items - 1) // n_chunk
        return 1 - half if backward else half

    x_in, pre_in, outs = [], [], []
    recv = None
    for tick in range(n_ticks):
        fresh = x_all[tick * n_tok:(tick + 1) * n_tok] if tick < n_chunk else None
        if recv is None:
            h_cur = fresh
        elif fresh is None:
            h_cur = recv
        else:
            h_cur = jnp.where(on_first, fresh, recv)
        w_one, w_two = weights(half_of(tick, False), half_of(tick - 1, False))
        pre = dot32(h_cur, w_one, ((1,), (0,)))
        act = gelu_tanh(pre).astype(jnp.bfloat16)
        h_out = (h_cur.astype(jnp.float32) + dot32(act, w_two, ((1,), (0,)))).astype(jnp.bfloat16)
        x_in.append(h_cur)
        outs.append(h_out)
        recv = lax.ppermute(h_out, "stage", swap)

    loss_acc = jnp.zeros((), jnp.float32)
    seeds = []
    for chunk in range(n_chunk):
        h_last = outs[n_chunk + chunk + 1]
        residual = h_last.astype(jnp.float32) - t_all[chunk * n_tok:(chunk + 1) * n_tok].astype(jnp.float32)
        loss_acc = loss_acc + 0.5 * jnp.sum(residual * residual)
        seeds.append((residual / n_tokens).astype(jnp.bfloat16))
    loss_acc = jnp.where(on_first, 0.0, loss_acc)

    g_in, r_in, a_in = [], [], []
    saved = []
    recv = None
    for tick in range(n_ticks):
        fresh = seeds[tick] if tick < n_chunk else None
        if recv is None:
            grad = fresh
        elif fresh is None:
            grad = recv
        else:
            grad = jnp.where(on_first, recv, fresh)
        first_item = min(max(tick - 1, 0), n_items - 1)
        second_item = min(tick, n_items - 1)
        w_one, w_two = weights(half_of(first_item, True), half_of(second_item, True))
        first_tick = half_of(first_item, True) * n_chunk + first_item % n_chunk
        second_tick = half_of(second_item, True) * n_chunk + second_item % n_chunk + 1
        if first_tick == second_tick:
            x_cur = x_in[first_tick]
        else:
            x_cur = jnp.where(on_first, x_in[first_tick], x_in[second_tick])
        pre = dot32(x_cur, w_one, ((1,), (0,)))
        act, pull = jax.vjp(gelu_tanh, pre)
        r_cur = pull(dot32(grad, w_two, ((1,), (1,))))[0].astype(jnp.bfloat16)
        back = (grad.astype(jnp.float32) + dot32(r_cur, w_one, ((1,), (1,)))).astype(jnp.bfloat16)
        g_in.append(grad)
        r_in.append(r_cur)
        a_in.append(act.astype(jnp.bfloat16))
        saved.append(x_cur)
        if tick < n_ticks - 1:
            recv = lax.ppermute(back, "stage", swap)

    def pick(per_tick, half):
        base = (1 - half) * n_chunk
        return jnp.concatenate([jnp.where(on_first, per_tick[base + c + 1], per_tick[base + c]) for c in range(n_chunk)], axis=0)

    grads = []
    for half in (1, 0):
        x_h, g_h, r_h, a_h = pick(saved, half), pick(g_in, half), pick(r_in, half), pick(a_in, half)
        grads.append((dot32(x_h, r_h, ((0,), (0,))), dot32(a_h, g_h, ((0,), (0,)))))
    return grads[1], grads[0], loss_acc


def solution(mesh):
    n_stage = mesh.shape["stage"]
    n_data = mesh.shape["data"]

    def device_step(x_loc, t_loc, w1_loc, w2_loc, wm_loc, m_loc, v_loc):
        n_micro, n_tok, d_model = x_loc.shape
        d_ff = w1_loc.shape[4]
        n_tokens = n_micro * n_tok * n_data
        n_blocks = 2 * n_stage
        tau_clip = 0.3 * d_model * math.sqrt(n_blocks * (3.0 / n_tokens + 0.008))
        learn_rate = 0.1 / math.sqrt(4.0 * d_model * n_blocks)
        first_kind = lax.axis_index("data") < n_data // 2
        x_all = x_loc.reshape(n_micro * n_tok, d_model)
        t_all = t_loc.reshape(n_micro * n_tok, d_model)
        grad_zero, grad_one, loss_acc = run_stack(x_all, t_all, w1_loc[0, :, 0], w2_loc[0, :, 0], n_tokens, 2)
        tiles = d_model * d_ff * 2 // n_data // 1024
        rows_one, rows_two = 2 * d_model // n_data, 2 * d_ff // n_data

        def scatter(pair):
            full = jnp.concatenate([to_tiles(pair[0]), to_tiles(pair[1])], axis=0).reshape(n_data, tiles, 8, 128)
            piece = lax.psum_scatter(full, "data", scatter_dimension=0, tiled=True)[0]
            return jnp.where(first_kind, from_tiles(piece, rows_one, d_ff).reshape(-1, 128), from_tiles(piece, rows_two, d_model).reshape(-1, 128))

        piece_one = scatter(grad_one)
        piece_zero = scatter(grad_zero)
        grad = jnp.stack([piece_zero, piece_one])
        sums = lax.psum(jnp.stack([jnp.sum(grad * grad), loss_acc]), ("stage", "data"))
        clip = jnp.minimum(1.0, tau_clip / jnp.sqrt(sums[0]))
        grad_clip = clip * grad.reshape(2, 1, -1)
        m_new = BETA_ONE * m_loc[0] + (1.0 - BETA_ONE) * grad_clip
        v_new = BETA_TWO * v_loc[0] + (1.0 - BETA_TWO) * grad_clip * grad_clip
        m_hat = m_new / (1.0 - BETA_ONE ** ADAM_STEP)
        v_hat = v_new / (1.0 - BETA_TWO ** ADAM_STEP)
        w_new = wm_loc[0] - learn_rate * (m_hat / (jnp.sqrt(v_hat) + ADAM_EPS) + WEIGHT_DECAY * wm_loc[0])
        w_bf = w_new.astype(jnp.bfloat16).reshape(2, -1)
        w_tiles = jnp.stack([jnp.where(first_kind, to_tiles(w_bf[h].reshape(rows_one, d_ff)), to_tiles(w_bf[h].reshape(rows_two, d_model))) for h in range(2)])
        w_full = lax.all_gather(w_tiles, "data", axis=1, tiled=False)
        half = n_data // 2
        w1_new = jnp.stack([from_tiles(w_full[h, :half], d_model, d_ff) for h in range(2)])[None, :, None]
        w2_new = jnp.stack([from_tiles(w_full[h, half:], d_ff, d_model) for h in range(2)])[None, :, None]
        return w1_new, w2_new, w_new[None], m_new[None], v_new[None], sums[1] / n_tokens

    act_spec = P(None, "data", None)
    flat_spec = P("stage", None, None, "data")
    return jax.shard_map(device_step, mesh=mesh, in_specs=(act_spec, act_spec, P("stage"), P("stage"), flat_spec, flat_spec, flat_spec), out_specs=(P("stage"), P("stage"), flat_spec, flat_spec, flat_spec, P()), check_vma=False)
```

```python
import functools
import math
import jax
import jax.numpy as jnp
from jax import lax
from jax.experimental import pallas as pl
from jax.experimental.pallas import tpu as pltpu
from jax.sharding import PartitionSpec as P

BETA_ONE = 0.9
BETA_TWO = 0.999
ADAM_EPS = 1e-8
WEIGHT_DECAY = 0.1
ADAM_STEP = 1000


def gelu_tanh(pre_act):
    return jax.nn.gelu(pre_act, approximate=True)


def dot32(lhs, rhs, dims):
    return lax.dot_general(lhs, rhs, (dims, ((), ())), preferred_element_type=jnp.float32)


def to_tiles(mat):
    rows, cols = mat.shape
    return mat.reshape(rows // 8, 8, cols // 128, 128).transpose(0, 2, 1, 3).reshape(-1, 8, 128)


def run_stack(x_all, t_all, w1_loc, w2_loc, n_tokens, n_chunk):
    stage_idx = lax.axis_index("stage")
    on_first = stage_idx == 0
    n_rows, d_model = x_all.shape
    n_tok = n_rows // n_chunk
    n_items = 2 * n_chunk
    n_ticks = n_items + 1
    swap = [(0, 1), (1, 0)]

    def weights(half_first, half_second):
        if half_first == half_second:
            return w1_loc[half_first], w2_loc[half_first]
        return (jnp.where(on_first, w1_loc[half_first], w1_loc[half_second]),
                jnp.where(on_first, w2_loc[half_first], w2_loc[half_second]))

    def half_of(item, backward):
        half = min(max(item, 0), n_items - 1) // n_chunk
        return 1 - half if backward else half

    x_in, pre_in, outs = [], [], []
    recv = None
    for tick in range(n_ticks):
        fresh = x_all[tick * n_tok:(tick + 1) * n_tok] if tick < n_chunk else None
        if recv is None:
            h_cur = fresh
        elif fresh is None:
            h_cur = recv
        else:
            h_cur = jnp.where(on_first, fresh, recv)
        w_one, w_two = weights(half_of(tick, False), half_of(tick - 1, False))
        pre = dot32(h_cur, w_one, ((1,), (0,)))
        act = gelu_tanh(pre).astype(jnp.bfloat16)
        h_out = (h_cur.astype(jnp.float32) + dot32(act, w_two, ((1,), (0,)))).astype(jnp.bfloat16)
        x_in.append(h_cur)
        outs.append(h_out)
        recv = lax.ppermute(h_out, "stage", swap)

    loss_acc = jnp.zeros((), jnp.float32)
    seeds = []
    for chunk in range(n_chunk):
        h_last = outs[n_chunk + chunk + 1]
        residual = h_last.astype(jnp.float32) - t_all[chunk * n_tok:(chunk + 1) * n_tok].astype(jnp.float32)
        loss_acc = loss_acc + 0.5 * jnp.sum(residual * residual)
        seeds.append((residual / n_tokens).astype(jnp.bfloat16))
    loss_acc = jnp.where(on_first, 0.0, loss_acc)

    g_in, r_in, a_in = [], [], []
    saved = []
    recv = None
    for tick in range(n_ticks):
        fresh = seeds[tick] if tick < n_chunk else None
        if recv is None:
            grad = fresh
        elif fresh is None:
            grad = recv
        else:
            grad = jnp.where(on_first, recv, fresh)
        first_item = min(max(tick - 1, 0), n_items - 1)
        second_item = min(tick, n_items - 1)
        w_one, w_two = weights(half_of(first_item, True), half_of(second_item, True))
        first_tick = half_of(first_item, True) * n_chunk + first_item % n_chunk
        second_tick = half_of(second_item, True) * n_chunk + second_item % n_chunk + 1
        if first_tick == second_tick:
            x_cur = x_in[first_tick]
        else:
            x_cur = jnp.where(on_first, x_in[first_tick], x_in[second_tick])
        pre = dot32(x_cur, w_one, ((1,), (0,)))
        act, pull = jax.vjp(gelu_tanh, pre)
        r_cur = pull(dot32(grad, w_two, ((1,), (1,))))[0].astype(jnp.bfloat16)
        back = (grad.astype(jnp.float32) + dot32(r_cur, w_one, ((1,), (1,)))).astype(jnp.bfloat16)
        g_in.append(grad)
        r_in.append(r_cur)
        a_in.append(act.astype(jnp.bfloat16))
        saved.append(x_cur)
        if tick < n_ticks - 1:
            recv = lax.ppermute(back, "stage", swap)

    def pick(per_tick, half):
        base = (1 - half) * n_chunk
        return jnp.concatenate([jnp.where(on_first, per_tick[base + c + 1], per_tick[base + c]) for c in range(n_chunk)], axis=0)

    grads = []
    for half in (1, 0):
        x_h, g_h, r_h, a_h = pick(saved, half), pick(g_in, half), pick(r_in, half), pick(a_in, half)
        grads.append((dot32(x_h, r_h, ((0,), (0,))), dot32(a_h, g_h, ((0,), (0,)))))
    return grads[1], grads[0], loss_acc


TILES = 72
PART = 24
ORDERS = ((2, 1, 0), (1, 0, 2), (0, 2, 1))
MESH_ID = pl.DeviceIdType.MESH


def tail_kernel(tau_clip, learn_rate, g0_ref, g1_ref, w_ref, m_ref, v_ref, loss_ref,
                w_out, m_out, v_out, stat_out, full_out,
                recv1, recv2, recv3, local, wbf, nbuf,
                s1, r1, s2, r2, s3, r3, l_sem, own_sem, ns, nr,
                t1, q1, t2, q2, t3, q3):
    stage = lax.axis_index("stage")
    me = lax.axis_index("data")
    coords = (me // 16, (me // 4) % 4, me % 4)
    strides = (16, 4, 1)
    g_refs = (g0_ref, g1_ref)
    streams = [(k, d) for k in range(3) for d in range(2)]

    def peer(axis, delta):
        moved = lax.rem(coords[axis] + delta + 4, 4)
        return (stage, me + (moved - coords[axis]) * strides[axis])

    def ring(axis, delta):
        return lax.rem(coords[axis] + delta + 8, 4)

    barrier = pltpu.get_barrier_semaphore()
    for axis in range(3):
        for delta in (1, 2, 3):
            pl.semaphore_signal(barrier, inc=1, device_id=peer(axis, delta), device_id_type=MESH_ID)
    pl.semaphore_signal(barrier, inc=1, device_id=(1 - stage, me), device_id_type=MESH_ID)
    pl.semaphore_wait(barrier, 10)

    def sgn(d):
        return 1 if d == 0 else -1

    def pick(k, on_a, on_b, on_c):
        index = [None] * 3
        index[ORDERS[k][0]], index[ORDERS[k][1]], index[ORDERS[k][2]] = on_a, on_b, on_c
        return tuple(index)

    def remote(src, dst, send_sem, recv_sem, target):
        return pltpu.make_async_remote_copy(src_ref=src, dst_ref=dst, send_sem=send_sem, recv_sem=recv_sem, device_id=target, device_id_type=MESH_ID)

    def grad_part(st, on_a, on_b):
        k, d = streams[st]
        return g_refs[d].at[pick(k, on_a, on_b, slice(None)) + (pl.ds(PART * k, PART),)]

    def sub_of(st, i):
        k, d = streams[st]
        return ring(ORDERS[k][1], -sgn(d) * (1 + i))

    def next_of(st, phase):
        k, d = streams[st]
        return peer(ORDERS[k][phase], sgn(d))

    def first_send(st, i):
        k, d = streams[st]
        return remote(grad_part(st, ring(ORDERS[k][0], -sgn(d)), sub_of(st, i)), recv1.at[st, 0, i], s1.at[st, 0, i], r1.at[st, 0, i], next_of(st, 0))

    def forward1(st, step, i):
        return remote(recv1.at[st, step, i], recv1.at[st, step + 1, i], s1.at[st, step + 1, i], r1.at[st, step + 1, i], next_of(st, 0))

    def arrived1(st, step, i):
        return remote(recv1.at[st, step, i], recv1.at[st, step, i], s1.at[st, step, i], r1.at[st, step, i], next_of(st, 0))

    def fetch(st, n):
        k, d = streams[st]
        step, i = n // 4, n % 4
        return pltpu.make_async_copy(grad_part(st, ring(ORDERS[k][0], -sgn(d) * (2 + step)), sub_of(st, i)), local.at[st, n % 2], l_sem.at[st, n % 2])

    def send2(st, step):
        src = recv1.at[st, 2, 0] if step == 0 else recv2.at[st, step - 1]
        return remote(src, recv2.at[st, step], s2.at[st, step], r2.at[st, step], next_of(st, 1))

    def send3(st, step):
        k, d = streams[st]
        src = recv2.at[st, 2, ring(ORDERS[k][2], -sgn(d))] if step == 0 else recv3.at[st, step - 1]
        return remote(src, recv3.at[st, step], s3.at[st, step], r3.at[st, step], next_of(st, 2))

    all_st = range(6)
    for st in all_st:
        for n in range(2):
            fetch(st, n).start()
    for i in range(4):
        for st in all_st:
            first_send(st, i).start()

    def accumulate(st, step, i, n, more):
        arrived1(st, step, i).wait_recv()
        fetch(st, n).wait()
        recv1[st, step, i] = recv1[st, step, i] + local[st, n % 2]
        if more:
            fetch(st, n + 2).start()

    def phase1(n, carry):
        step, i = n // 4, n % 4
        for st in all_st:
            accumulate(st, step, i, n, True)
            forward1(st, step, i).start()
        return carry

    lax.fori_loop(0, 8, phase1, 0)
    for i in range(4):
        for st in all_st:
            accumulate(st, 2, i, 8 + i, i < 2)
            if i == 0:
                send2(st, 0).start()
        if i > 0:
            for st in all_st:
                send2(st, i - 1).wait_recv()
                recv2[st, i - 1] = recv2[st, i - 1] + recv1[st, 2, i]
                if i < 3:
                    send2(st, i).start()
                else:
                    send3(st, 0).start()
    for step in range(3):
        for st in all_st:
            k, d = streams[st]
            send3(st, step).wait_recv()
            recv3[st, step] = recv3[st, step] + recv2[st, 2, ring(ORDERS[k][2], -sgn(d) * (2 + step))]
            if step < 2:
                send3(st, step + 1).start()

    total = jnp.zeros((8, 128), jnp.float32)
    for st in all_st:
        piece = recv3[st, 2]
        total = total + jnp.sum(piece * piece, axis=0)

    parts = (total, loss_ref[...])
    for phase in range(4):
        size = 2 if phase == 0 else 4
        mine = stage if phase == 0 else coords[phase - 1]
        nbuf[phase, mine, 0] = parts[0]
        nbuf[phase, mine, 1] = parts[1]
        sends = []
        for delta in range(1, size):
            target = (1 - stage, me) if phase == 0 else peer(phase - 1, delta)
            sends.append(remote(nbuf.at[phase, mine], nbuf.at[phase, mine], ns.at[phase, delta], nr.at[phase, delta], target))
        for send in sends:
            send.start()
        for send in sends:
            send.wait_recv()
        parts = tuple(sum((nbuf[phase, slot, j] for slot in range(1, size)), nbuf[phase, 0, j]) for j in range(2))
        for send in sends:
            send.wait_send()

    stat_out[...] = jnp.full((8, 128), jnp.sum(parts[1]), jnp.float32)
    norm = jnp.sqrt(jnp.full((8, 128), jnp.sum(parts[0]), jnp.float32))
    clip = jnp.minimum(1.0, tau_clip / norm)

    def update(width):
        def group(k, carry):
            for h in range(2):
                for t in range(PART):
                    rows = pl.ds(k * 192 + (t // width) * (8 * width) + t % width, 8, stride=width)
                    grad = clip * recv3[2 * k + h, 2, t]
                    m_new = BETA_ONE * m_ref[h, rows, :] + (1.0 - BETA_ONE) * grad
                    v_new = BETA_TWO * v_ref[h, rows, :] + (1.0 - BETA_TWO) * grad * grad
                    m_hat = m_new / (1.0 - BETA_ONE ** ADAM_STEP)
                    v_hat = v_new / (1.0 - BETA_TWO ** ADAM_STEP)
                    w_old = w_ref[h, rows, :]
                    w_new = w_old - learn_rate * (m_hat / (jnp.sqrt(v_hat) + ADAM_EPS) + WEIGHT_DECAY * w_old)
                    w_out[h, rows, :] = w_new
                    m_out[h, rows, :] = m_new
                    v_out[h, rows, :] = v_new
                    wbf[h, k * PART + t] = w_new.astype(jnp.bfloat16)
            return carry

        lax.fori_loop(0, 3, group, 0)

    @pl.when(me < 32)
    def _():
        update(24)

    @pl.when(me >= 32)
    def _():
        update(6)

    def full_part(st, on_a, on_b, on_c):
        k, d = streams[st]
        return full_out.at[(d,) + pick(k, on_a, on_b, on_c) + (pl.ds(PART * k, PART),)]

    def coord_of(st, phase, delta):
        k, d = streams[st]
        return ring(ORDERS[k][phase], -sgn(d) * delta)

    def gather1(st, step):
        k, d = streams[st]
        place = full_part(st, coord_of(st, 0, 0), coord_of(st, 1, 0), coord_of(st, 2, step))
        src = wbf.at[d, pl.ds(PART * k, PART)] if step == 0 else place
        return remote(src, place, t1.at[st, step], q1.at[st, step], next_of(st, 2))

    def gather2(st, step):
        place = full_part(st, coord_of(st, 0, 0), coord_of(st, 1, step), slice(None))
        return remote(place, place, t2.at[st, step], q2.at[st, step], next_of(st, 1))

    def gather3(st, step, i):
        place = full_part(st, coord_of(st, 0, step), coord_of(st, 1, i), slice(None))
        return remote(place, place, t3.at[st, step, i], q3.at[st, step, i], next_of(st, 0))

    def own(st):
        k, d = streams[st]
        return pltpu.make_async_copy(wbf.at[d, pl.ds(PART * k, PART)], full_part(st, coord_of(st, 0, 0), coord_of(st, 1, 0), coord_of(st, 2, 0)), own_sem.at[st])

    for st in all_st:
        gather1(st, 0).start()
        own(st).start()
    for step in range(3):
        for st in all_st:
            gather1(st, step).wait_recv()
            if step < 2:
                gather1(st, step + 1).start()
    for st in all_st:
        own(st).wait()
        gather2(st, 0).start()
        gather3(st, 0, 0).start()
    for step in range(3):
        for st in all_st:
            gather2(st, step).wait_recv()
            if step < 2:
                gather2(st, step + 1).start()
            gather3(st, 0, step + 1).start()

    def phase3(n, carry):
        step, i = n // 4, n % 4
        for st in all_st:
            gather3(st, step, i).wait_recv()
            gather3(st, step + 1, i).start()
        return carry

    lax.fori_loop(0, 8, phase3, 0)
    for i in range(4):
        for st in all_st:
            gather3(st, 2, i).wait_recv()

    def drain(n, carry):
        step, i = n // 4, n % 4
        for st in all_st:
            arrived1(st, step, i).wait_send()
            gather3(st, step, i).wait_send()
        return carry

    lax.fori_loop(0, 12, drain, 0)
    for step in range(3):
        for st in all_st:
            send2(st, step).wait_send()
            send3(st, step).wait_send()
            gather1(st, step).wait_send()
            gather2(st, step).wait_send()


def tail(g0, g1, w_flat, m_flat, v_flat, loss_tile, tau_clip, learn_rate):
    flat = jax.ShapeDtypeStruct((2, 576, 128), jnp.float32)
    in_vmem = pl.BlockSpec(memory_space=pltpu.VMEM)
    in_any = pl.BlockSpec(memory_space=pl.ANY)
    dma = pltpu.SemaphoreType.DMA
    return pl.pallas_call(
        functools.partial(tail_kernel, tau_clip, learn_rate),
        out_shape=(flat, flat, flat, jax.ShapeDtypeStruct((8, 128), jnp.float32), jax.ShapeDtypeStruct((2, 4, 4, 4, TILES, 8, 128), jnp.bfloat16)),
        in_specs=[in_any] * 2 + [in_vmem] * 4,
        out_specs=(in_vmem, in_vmem, in_vmem, in_vmem, in_any),
        scratch_shapes=[
            pltpu.VMEM((6, 3, 4, 4, PART, 8, 128), jnp.float32),
            pltpu.VMEM((6, 3, 4, PART, 8, 128), jnp.float32),
            pltpu.VMEM((6, 3, PART, 8, 128), jnp.float32),
            pltpu.VMEM((6, 2, 4, PART, 8, 128), jnp.float32),
            pltpu.VMEM((2, TILES, 8, 128), jnp.bfloat16),
            pltpu.VMEM((4, 4, 2, 8, 128), jnp.float32),
            dma((6, 3, 4)), dma((6, 3, 4)), dma((6, 3)), dma((6, 3)), dma((6, 3)), dma((6, 3)),
            dma((6, 2)), dma((6,)), dma((4, 4)), dma((4, 4)),
            dma((6, 3)), dma((6, 3)), dma((6, 3)), dma((6, 3)), dma((6, 3, 4)), dma((6, 3, 4)),
        ],
        compiler_params=pltpu.CompilerParams(collective_id=1, has_side_effects=True, vmem_limit_bytes=60 * 1024 * 1024),
        name="tail",
    )(g0, g1, w_flat, m_flat, v_flat, loss_tile)


def solution(mesh):
    n_stage = mesh.shape["stage"]
    n_data = mesh.shape["data"]

    def device_step(x_loc, t_loc, w1_loc, w2_loc, wm_loc, m_loc, v_loc):
        n_micro, n_tok, d_model = x_loc.shape
        d_ff = w1_loc.shape[4]
        n_tokens = n_micro * n_tok * n_data
        n_blocks = 2 * n_stage
        tau_clip = 0.3 * d_model * math.sqrt(n_blocks * (3.0 / n_tokens + 0.008))
        learn_rate = 0.1 / math.sqrt(4.0 * d_model * n_blocks)
        x_all = x_loc.reshape(n_micro * n_tok, d_model)
        t_all = t_loc.reshape(n_micro * n_tok, d_model)
        grad_zero, grad_one, loss_acc = run_stack(x_all, t_all, w1_loc[0, :, 0], w2_loc[0, :, 0], n_tokens, 2)

        def whole(pair):
            return jnp.concatenate([to_tiles(pair[0]), to_tiles(pair[1])], axis=0).reshape(4, 4, 4, TILES, 8, 128)

        loss_tile = jnp.where(lax.broadcasted_iota(jnp.int32, (8, 128), 0) + lax.broadcasted_iota(jnp.int32, (8, 128), 1) == 0, loss_acc, 0.0)
        w_new, m_new, v_new, stat, w_full = tail(
            whole(grad_zero), whole(grad_one), wm_loc.reshape(2, 576, 128), m_loc.reshape(2, 576, 128), v_loc.reshape(2, 576, 128),
            loss_tile, tau_clip, learn_rate)
        w1_new = w_full[:, :2].reshape(2, d_model // 8, d_ff // 128, 8, 128).transpose(0, 1, 3, 2, 4).reshape(1, 2, 1, d_model, d_ff)
        w2_new = w_full[:, 2:].reshape(2, d_ff // 8, d_model // 128, 8, 128).transpose(0, 1, 3, 2, 4).reshape(1, 2, 1, d_ff, d_model)
        flat_dims = (1, 2, 1, -1)
        return w1_new, w2_new, w_new.reshape(flat_dims), m_new.reshape(flat_dims), v_new.reshape(flat_dims), stat[0, 0] / n_tokens

    act_spec = P(None, "data", None)
    flat_spec = P("stage", None, None, "data")
    return jax.shard_map(device_step, mesh=mesh, in_specs=(act_spec, act_spec, P("stage"), P("stage"), flat_spec, flat_spec, flat_spec), out_specs=(P("stage"), P("stage"), flat_spec, flat_spec, flat_spec, P()), check_vma=False)
```

```python
import functools
import math
import jax
import jax.numpy as jnp
from jax import lax
from jax.experimental import pallas as pl
from jax.experimental.pallas import tpu as pltpu
from jax.sharding import PartitionSpec as P

BETA_ONE = 0.9
BETA_TWO = 0.999
ADAM_EPS = 1e-8
WEIGHT_DECAY = 0.1
ADAM_STEP = 1000


TILE = (8, 128)
TILES = 72
VMEM_LIMIT = 60 * 1024 * 1024
PART = 24
ORDERS = ((2, 1, 0), (1, 0, 2), (0, 2, 1))
MESH_ID = pl.DeviceIdType.MESH


def tail_kernel(tau_clip, learn_rate, g_ref, w_ref, m_ref, v_ref, loss_ref,
                w_out, m_out, v_out, stat_out, full_out,
                recv1, recv2, recv3, local, wbf, nbuf,
                s1, r1, s2, r2, s3, r3, l_sem, own_sem, ns, nr,
                t1, q1, t2, q2, t3, q3):
    stage = lax.axis_index("stage")
    me = lax.axis_index("data")
    coords = (me // 16, (me // 4) % 4, me % 4)
    strides = (16, 4, 1)
    g_refs = (g_ref.at[0], g_ref.at[1])
    streams = [(k, d) for k in range(3) for d in range(2)]

    def peer(axis, delta):
        moved = lax.rem(coords[axis] + delta + 4, 4)
        return (stage, me + (moved - coords[axis]) * strides[axis])

    def ring(axis, delta):
        return lax.rem(coords[axis] + delta + 8, 4)

    barrier = pltpu.get_barrier_semaphore()
    for axis in range(3):
        for delta in (1, 2, 3):
            pl.semaphore_signal(barrier, inc=1, device_id=peer(axis, delta), device_id_type=MESH_ID)
    pl.semaphore_signal(barrier, inc=1, device_id=(1 - stage, me), device_id_type=MESH_ID)
    pl.semaphore_wait(barrier, 10)

    def sgn(d):
        return 1 if d == 0 else -1

    def pick(k, on_a, on_b, on_c):
        index = [None] * 3
        index[ORDERS[k][0]], index[ORDERS[k][1]], index[ORDERS[k][2]] = on_a, on_b, on_c
        return tuple(index)

    def remote(src, dst, send_sem, recv_sem, target):
        return pltpu.make_async_remote_copy(src_ref=src, dst_ref=dst, send_sem=send_sem, recv_sem=recv_sem, device_id=target, device_id_type=MESH_ID)

    def grad_part(st, on_a, on_b):
        k, d = streams[st]
        return g_refs[d].at[pick(k, on_a, on_b, slice(None)) + (pl.ds(PART * k, PART),)]

    def sub_of(st, i):
        k, d = streams[st]
        return ring(ORDERS[k][1], -sgn(d) * (1 + i))

    def next_of(st, phase):
        k, d = streams[st]
        return peer(ORDERS[k][phase], sgn(d))

    def first_send(st, i):
        k, d = streams[st]
        return remote(grad_part(st, ring(ORDERS[k][0], -sgn(d)), sub_of(st, i)), recv1.at[st, 0, i], s1.at[st, 0, i], r1.at[st, 0, i], next_of(st, 0))

    def forward1(st, step, i):
        return remote(recv1.at[st, step, i], recv1.at[st, step + 1, i], s1.at[st, step + 1, i], r1.at[st, step + 1, i], next_of(st, 0))

    def arrived1(st, step, i):
        return remote(recv1.at[st, step, i], recv1.at[st, step, i], s1.at[st, step, i], r1.at[st, step, i], next_of(st, 0))

    def fetch(st, n):
        k, d = streams[st]
        step, i = n // 4, n % 4
        return pltpu.make_async_copy(grad_part(st, ring(ORDERS[k][0], -sgn(d) * (2 + step)), sub_of(st, i)), local.at[st, n % 2], l_sem.at[st, n % 2])

    def send2(st, step):
        src = recv1.at[st, 2, 0] if step == 0 else recv2.at[st, step - 1]
        return remote(src, recv2.at[st, step], s2.at[st, step], r2.at[st, step], next_of(st, 1))

    def send3(st, step):
        k, d = streams[st]
        src = recv2.at[st, 2, ring(ORDERS[k][2], -sgn(d))] if step == 0 else recv3.at[st, step - 1]
        return remote(src, recv3.at[st, step], s3.at[st, step], r3.at[st, step], next_of(st, 2))

    all_st = range(6)
    for st in all_st:
        for n in range(2):
            fetch(st, n).start()
    for i in range(4):
        for st in all_st:
            first_send(st, i).start()

    def accumulate(st, step, i, n, more):
        arrived1(st, step, i).wait_recv()
        fetch(st, n).wait()
        recv1[st, step, i] = recv1[st, step, i] + local[st, n % 2]
        if more:
            fetch(st, n + 2).start()

    def phase1(n, carry):
        step, i = n // 4, n % 4
        for st in all_st:
            accumulate(st, step, i, n, True)
            forward1(st, step, i).start()
        return carry

    lax.fori_loop(0, 8, phase1, 0)
    for i in range(4):
        for st in all_st:
            accumulate(st, 2, i, 8 + i, i < 2)
            if i == 0:
                send2(st, 0).start()
        if i > 0:
            for st in all_st:
                send2(st, i - 1).wait_recv()
                recv2[st, i - 1] = recv2[st, i - 1] + recv1[st, 2, i]
                if i < 3:
                    send2(st, i).start()
                else:
                    send3(st, 0).start()
    for step in range(3):
        for st in all_st:
            k, d = streams[st]
            send3(st, step).wait_recv()
            recv3[st, step] = recv3[st, step] + recv2[st, 2, ring(ORDERS[k][2], -sgn(d) * (2 + step))]
            if step < 2:
                send3(st, step + 1).start()

    total = jnp.zeros((8, 128), jnp.float32)
    for st in all_st:
        piece = recv3[st, 2]
        total = total + jnp.sum(piece * piece, axis=0)

    parts = (total, loss_ref[...])
    for phase in range(4):
        size = 2 if phase == 0 else 4
        mine = stage if phase == 0 else coords[phase - 1]
        nbuf[phase, mine, 0] = parts[0]
        nbuf[phase, mine, 1] = parts[1]
        sends = []
        for delta in range(1, size):
            target = (1 - stage, me) if phase == 0 else peer(phase - 1, delta)
            sends.append(remote(nbuf.at[phase, mine], nbuf.at[phase, mine], ns.at[phase, delta], nr.at[phase, delta], target))
        for send in sends:
            send.start()
        for send in sends:
            send.wait_recv()
        parts = tuple(sum((nbuf[phase, slot, j] for slot in range(1, size)), nbuf[phase, 0, j]) for j in range(2))
        for send in sends:
            send.wait_send()

    stat_out[...] = jnp.full((8, 128), jnp.sum(parts[1]), jnp.float32)
    norm = jnp.sqrt(jnp.full((8, 128), jnp.sum(parts[0]), jnp.float32))
    clip = jnp.minimum(1.0, tau_clip / norm)

    def update(width):
        def group(k, carry):
            for h in range(2):
                for t in range(PART):
                    rows = pl.ds(k * 192 + (t // width) * (8 * width) + t % width, 8, stride=width)
                    grad = clip * recv3[2 * k + h, 2, t]
                    m_new = BETA_ONE * m_ref[h, rows, :] + (1.0 - BETA_ONE) * grad
                    v_new = BETA_TWO * v_ref[h, rows, :] + (1.0 - BETA_TWO) * grad * grad
                    m_hat = m_new / (1.0 - BETA_ONE ** ADAM_STEP)
                    v_hat = v_new / (1.0 - BETA_TWO ** ADAM_STEP)
                    w_old = w_ref[h, rows, :]
                    w_new = w_old - learn_rate * (m_hat / (jnp.sqrt(v_hat) + ADAM_EPS) + WEIGHT_DECAY * w_old)
                    w_out[h, rows, :] = w_new
                    m_out[h, rows, :] = m_new
                    v_out[h, rows, :] = v_new
                    wbf[h, k * PART + t] = w_new.astype(jnp.bfloat16)
            return carry

        lax.fori_loop(0, 3, group, 0)

    @pl.when(me < 32)
    def _():
        update(24)

    @pl.when(me >= 32)
    def _():
        update(6)

    def full_part(st, on_a, on_b, on_c):
        k, d = streams[st]
        return full_out.at[(d,) + pick(k, on_a, on_b, on_c) + (pl.ds(PART * k, PART),)]

    def coord_of(st, phase, delta):
        k, d = streams[st]
        return ring(ORDERS[k][phase], -sgn(d) * delta)

    def gather1(st, step):
        k, d = streams[st]
        place = full_part(st, coord_of(st, 0, 0), coord_of(st, 1, 0), coord_of(st, 2, step))
        src = wbf.at[d, pl.ds(PART * k, PART)] if step == 0 else place
        return remote(src, place, t1.at[st, step], q1.at[st, step], next_of(st, 2))

    def gather2(st, step):
        place = full_part(st, coord_of(st, 0, 0), coord_of(st, 1, step), slice(None))
        return remote(place, place, t2.at[st, step], q2.at[st, step], next_of(st, 1))

    def gather3(st, step, i):
        place = full_part(st, coord_of(st, 0, step), coord_of(st, 1, i), slice(None))
        return remote(place, place, t3.at[st, step, i], q3.at[st, step, i], next_of(st, 0))

    def own(st):
        k, d = streams[st]
        return pltpu.make_async_copy(wbf.at[d, pl.ds(PART * k, PART)], full_part(st, coord_of(st, 0, 0), coord_of(st, 1, 0), coord_of(st, 2, 0)), own_sem.at[st])

    for st in all_st:
        gather1(st, 0).start()
        own(st).start()
    for step in range(3):
        for st in all_st:
            gather1(st, step).wait_recv()
            if step < 2:
                gather1(st, step + 1).start()
    for st in all_st:
        own(st).wait()
        gather2(st, 0).start()
        gather3(st, 0, 0).start()
    for step in range(3):
        for st in all_st:
            gather2(st, step).wait_recv()
            if step < 2:
                gather2(st, step + 1).start()
            gather3(st, 0, step + 1).start()

    def phase3(n, carry):
        step, i = n // 4, n % 4
        for st in all_st:
            gather3(st, step, i).wait_recv()
            gather3(st, step + 1, i).start()
        return carry

    lax.fori_loop(0, 8, phase3, 0)
    for i in range(4):
        for st in all_st:
            gather3(st, 2, i).wait_recv()

    def drain(n, carry):
        step, i = n // 4, n % 4
        for st in all_st:
            arrived1(st, step, i).wait_send()
            gather3(st, step, i).wait_send()
        return carry

    lax.fori_loop(0, 12, drain, 0)
    for step in range(3):
        for st in all_st:
            send2(st, step).wait_send()
            send3(st, step).wait_send()
            gather1(st, step).wait_send()
            gather2(st, step).wait_send()


def tail(grads, w_flat, m_flat, v_flat, loss_tile, tau_clip, learn_rate):
    f32, bf16 = jnp.float32, jnp.bfloat16
    flat = jax.ShapeDtypeStruct(w_flat.shape, f32)
    in_vmem = pl.BlockSpec(memory_space=pltpu.VMEM)
    in_any = pl.BlockSpec(memory_space=pl.ANY)
    dma = pltpu.SemaphoreType.DMA
    per_step = (6, 3)
    per_sub = per_step + (4,)
    part = (PART,) + TILE
    return pl.pallas_call(
        functools.partial(tail_kernel, tau_clip, learn_rate),
        out_shape=(flat, flat, flat, jax.ShapeDtypeStruct(TILE, f32), jax.ShapeDtypeStruct(grads.shape, bf16)),
        in_specs=[in_any] + [in_vmem] * 4,
        out_specs=(in_vmem, in_vmem, in_vmem, in_vmem, in_any),
        scratch_shapes=[
            pltpu.VMEM(per_sub + (4,) + part, f32),
            pltpu.VMEM(per_sub + part, f32),
            pltpu.VMEM(per_step + part, f32),
            pltpu.VMEM((6, 2, 4) + part, f32),
            pltpu.VMEM((2, TILES) + TILE, bf16),
            pltpu.VMEM((4, 4, 2) + TILE, f32),
            *[dma(per_sub)] * 2, *[dma(per_step)] * 4,
            dma((6, 2)), dma((6,)), *[dma((4, 4))] * 2,
            *[dma(per_step)] * 4, *[dma(per_sub)] * 2,
        ],
        compiler_params=pltpu.CompilerParams(collective_id=1, has_side_effects=True, vmem_limit_bytes=VMEM_LIMIT),
        name="tail",
    )(grads, w_flat, m_flat, v_flat, loss_tile)


ROWS = 256
GELU_K = math.sqrt(2.0 / math.pi)
GELU_C = 0.044715


def stack_kernel(n_tokens, x_hbm, t_hbm, w1_hbm, w2_hbm, g_out, loss_out,
                 w1, w2, xs, gs, us, acts, rs, outf, outb, tgt, stage1, stage2,
                 w1_sem, w2_sem, x_sem, t_sem, xsend, xrecv, gsend, grecv, o1_sem, o2_sem):
    stage = lax.axis_index("stage")
    me = lax.axis_index("data")
    partner = (1 - stage, me)
    n_half, d_model, d_ff = w1.shape

    def load_w1(h):
        return pltpu.make_async_copy(w1_hbm.at[h], w1.at[h], w1_sem.at[h])

    def load_w2(h):
        return pltpu.make_async_copy(w2_hbm.at[h], w2.at[h], w2_sem.at[h])

    load_x = pltpu.make_async_copy(x_hbm, xs.at[0], x_sem)
    load_t = pltpu.make_async_copy(t_hbm, tgt, t_sem)

    @pl.when(stage == 0)
    def _():
        load_x.start()

    load_w1(0).start()
    load_w2(0).start()
    load_w1(1).start()
    load_w2(1).start()
    load_t.start()

    barrier = pltpu.get_barrier_semaphore()
    pl.semaphore_signal(barrier, inc=1, device_id=partner, device_id_type=MESH_ID)
    pl.semaphore_wait(barrier, 1)

    @pl.when(stage == 0)
    def _():
        load_x.wait()

    loss_out[...] = jnp.zeros((8, 128), jnp.float32)

    def dot(lhs, rhs, on_left, on_right):
        return lax.dot_general(lhs, rhs, (((on_left,), (on_right,)), ((), ())), preferred_element_type=jnp.float32)

    def rows_of(c):
        return pl.ds(pl.multiple_of(c * ROWS, ROWS), ROWS)

    def block(i, size):
        return pl.ds(pl.multiple_of(i * size, size), size)

    def send_x(h, c):
        return pltpu.make_async_remote_copy(src_ref=outf.at[h, c], dst_ref=xs.at[h + stage, rows_of(c)], send_sem=xsend.at[h, c], recv_sem=xrecv.at[h + stage, c], device_id=partner, device_id_type=MESH_ID)

    def wait_x(h, c):
        pltpu.make_async_remote_copy(src_ref=outf.at[h, c], dst_ref=xs.at[h, rows_of(c)], send_sem=xsend.at[h, c], recv_sem=xrecv.at[h, c], device_id=partner, device_id_type=MESH_ID).wait_recv()

    def send_g(h, c):
        to = h - 1 + stage
        return pltpu.make_async_remote_copy(src_ref=outb.at[h, c], dst_ref=gs.at[to, rows_of(c)], send_sem=gsend.at[h, c], recv_sem=grecv.at[to, c], device_id=partner, device_id_type=MESH_ID)

    def wait_g(h, c):
        pltpu.make_async_remote_copy(src_ref=outb.at[h, c], dst_ref=gs.at[h, rows_of(c)], send_sem=gsend.at[h, c], recv_sem=grecv.at[h, c], device_id=partner, device_id_type=MESH_ID).wait_recv()

    def forward(item, carry):
        h, c = item // 2, item % 2
        rows = rows_of(c)

        @pl.when(c == 0)
        def _():
            load_w1(h).wait()
            load_w2(h).wait()

        @pl.when(h + stage > 0)
        def _():
            wait_x(h, c)

        def up(f, inner):
            cols = block(f, 512)
            pre = dot(xs[h, rows, :], w1[h, :, cols], 1, 0)
            us[h, rows, cols] = pre
            cdf = 0.5 * (1.0 + jnp.tanh(GELU_K * (pre + GELU_C * (pre * pre * pre))))
            acts[h, rows, cols] = (pre * cdf).astype(jnp.bfloat16)
            return inner

        lax.fori_loop(0, d_ff // 512, up, 0)

        def down(n, inner):
            cols = block(n, 256)
            val = dot(acts[h, rows, :], w2[h, :, cols], 1, 0)
            outf[h, c, :, cols] = (xs[h, rows, cols].astype(jnp.float32) + val).astype(jnp.bfloat16)
            return inner

        lax.fori_loop(0, d_model // 256, down, 0)

        @pl.when(h + stage < 2)
        def _():
            send_x(h, c).start()

        @pl.when(h + stage == 2)
        def _():
            @pl.when(c == 0)
            def _():
                load_t.wait()

            residual = outf[h, c].astype(jnp.float32) - tgt[rows, :].astype(jnp.float32)
            gs[h, rows, :] = (residual / n_tokens).astype(jnp.bfloat16)
            square = residual * residual
            part = sum(square[:, 128 * j:128 * (j + 1)] for j in range(d_model // 128))
            loss_out[...] += 0.5 * jnp.sum(part.reshape(ROWS // 8, 8, 128), axis=0)

        return carry

    lax.fori_loop(0, 2 * n_half, forward, 0)

    @pl.when(stage == 0)
    def _():
        load_t.wait()

    def out_one(h, n, i):
        return pltpu.make_async_copy(stage1.at[n % 2, i], g_out.at[h, pl.ds(0, 32), pl.ds(i * 24 + 2 * n, 2)], o1_sem.at[n % 2, i])

    def out_two(h, m):
        return pltpu.make_async_copy(stage2.at[m % 2], g_out.at[h, pl.ds(32 + 4 * m, 4)], o2_sem.at[m % 2])

    def backward(b, carry):
        h = 1 - b

        def chain(c, inner):
            rows = rows_of(c)

            @pl.when(h + stage < 2)
            def _():
                wait_g(h, c)

            def up(f, deep):
                cols = block(f, 512)
                q = dot(gs[h, rows, :], w2[h, cols, :], 1, 1)
                pre = us[h, rows, cols]
                square = pre * pre
                th = jnp.tanh(GELU_K * (pre + GELU_C * (square * pre)))
                slope = 0.5 * (1.0 + th) + 0.5 * pre * (1.0 - th * th) * (GELU_K * (1.0 + 3.0 * GELU_C * square))
                rs[rows, cols] = (q * slope).astype(jnp.bfloat16)
                return deep

            lax.fori_loop(0, d_ff // 512, up, 0)

            @pl.when(h + stage > 0)
            def _():
                def down(n, deep):
                    cols = block(n, 256)
                    val = dot(rs[rows, :], w1[h, cols, :], 1, 1)
                    outb[h, c, :, cols] = (gs[h, rows, cols].astype(jnp.float32) + val).astype(jnp.bfloat16)
                    return deep

                lax.fori_loop(0, d_model // 256, down, 0)
                send_g(h, c).start()

            return inner

        lax.fori_loop(0, 2, chain, 0)

        def grad_one(n, inner):
            @pl.when(b * 12 + n >= 2)
            def _():
                for i in range(3):
                    out_one(h, n, i).wait()

            val = dot(xs[h], rs[:, block(n, 256)], 0, 0)
            for p in range(32):
                for i in range(3):
                    for j in range(2):
                        stage1[n % 2, i, p, j] = val[p * 24 + i * 8:p * 24 + i * 8 + 8, 128 * j:128 * (j + 1)]
            for i in range(3):
                out_one(h, n, i).start()
            return inner

        lax.fori_loop(0, d_ff // 256, grad_one, 0)

        def grad_two(m, inner):
            @pl.when(b * 8 + m >= 2)
            def _():
                out_two(h, m).wait()

            val = dot(acts[h, :, block(m, 384)], gs[h], 0, 0)
            for p in range(4):
                for i in range(12):
                    for j in range(6):
                        stage2[m % 2, p, i * 6 + j] = val[p * 96 + i * 8:p * 96 + i * 8 + 8, 128 * j:128 * (j + 1)]
            out_two(h, m).start()
            return inner

        lax.fori_loop(0, d_ff // 384, grad_two, 0)
        return carry

    lax.fori_loop(0, n_half, backward, 0)
    for n in range(2):
        for i in range(3):
            out_one(0, n, i).wait()
        out_two(0, n).wait()

    for h in range(2):
        for c in range(2):
            @pl.when(h + stage < 2)
            def _():
                send_x(h, c).wait_send()

            @pl.when(h + stage > 0)
            def _():
                send_g(h, c).wait_send()


def stack(x_all, t_all, w1, w2, n_tokens):
    rows, d_model = x_all.shape
    d_ff = w1.shape[2]
    bf16, f32 = jnp.bfloat16, jnp.float32
    dma = pltpu.SemaphoreType.DMA
    in_any = pl.BlockSpec(memory_space=pl.ANY)
    return pl.pallas_call(
        functools.partial(stack_kernel, n_tokens),
        out_shape=(jax.ShapeDtypeStruct((2, 64, TILES, 8, 128), f32), jax.ShapeDtypeStruct((8, 128), f32)),
        in_specs=[in_any] * 4,
        out_specs=(in_any, pl.BlockSpec(memory_space=pltpu.VMEM)),
        scratch_shapes=[
            pltpu.VMEM((2, d_model, d_ff), bf16), pltpu.VMEM((2, d_ff, d_model), bf16),
            pltpu.VMEM((2, rows, d_model), bf16), pltpu.VMEM((2, rows, d_model), bf16),
            pltpu.VMEM((2, rows, d_ff), f32), pltpu.VMEM((2, rows, d_ff), bf16), pltpu.VMEM((rows, d_ff), bf16),
            pltpu.VMEM((2, 2, ROWS, d_model), bf16), pltpu.VMEM((2, 2, ROWS, d_model), bf16), pltpu.VMEM((rows, d_model), bf16),
            pltpu.VMEM((2, 3, 32, 2, 8, 128), f32), pltpu.VMEM((2, 4, TILES, 8, 128), f32),
            dma((2,)), dma((2,)), dma, dma, *[dma((2, 2))] * 4, dma((2, 3)), dma((2,)),
        ],
        compiler_params=pltpu.CompilerParams(collective_id=0, has_side_effects=True, vmem_limit_bytes=VMEM_LIMIT),
        name="stack",
    )(x_all, t_all, w1, w2)


def solution(mesh):
    n_stage = mesh.shape["stage"]
    n_data = mesh.shape["data"]

    def device_step(x_loc, t_loc, w1_loc, w2_loc, wm_loc, m_loc, v_loc):
        n_micro, n_tok, d_model = x_loc.shape
        d_ff = w1_loc.shape[4]
        n_tokens = n_micro * n_tok * n_data
        n_blocks = 2 * n_stage
        tau_clip = 0.3 * d_model * math.sqrt(n_blocks * (3.0 / n_tokens + 0.008))
        learn_rate = 0.1 / math.sqrt(4.0 * d_model * n_blocks)
        x_all = x_loc.reshape(n_micro * n_tok, d_model)
        t_all = t_loc.reshape(n_micro * n_tok, d_model)
        grads, loss_tile = stack(x_all, t_all, w1_loc[0, :, 0], w2_loc[0, :, 0], n_tokens)
        w_new, m_new, v_new, stat, w_full = tail(
            grads.reshape(2, 4, 4, 4, TILES, 8, 128), wm_loc.reshape(2, 576, 128), m_loc.reshape(2, 576, 128), v_loc.reshape(2, 576, 128),
            loss_tile, tau_clip, learn_rate)
        w1_new = w_full[:, :2].reshape(2, d_model // 8, d_ff // 128, 8, 128).transpose(0, 1, 3, 2, 4).reshape(1, 2, 1, d_model, d_ff)
        w2_new = w_full[:, 2:].reshape(2, d_ff // 8, d_model // 128, 8, 128).transpose(0, 1, 3, 2, 4).reshape(1, 2, 1, d_ff, d_model)
        flat_dims = (1, 2, 1, -1)
        return w1_new, w2_new, w_new.reshape(flat_dims), m_new.reshape(flat_dims), v_new.reshape(flat_dims), stat[0, 0] / n_tokens

    act_spec = P(None, "data", None)
    flat_spec = P("stage", None, None, "data")
    return jax.shard_map(device_step, mesh=mesh, in_specs=(act_spec, act_spec, P("stage"), P("stage"), flat_spec, flat_spec, flat_spec), out_specs=(P("stage"), P("stage"), flat_spec, flat_spec, flat_spec, P()), check_vma=False)
```

```python
import functools
import math
import jax
import jax.numpy as jnp
from jax import lax
from jax.experimental import pallas as pl
from jax.experimental.pallas import tpu as pltpu
from jax.sharding import PartitionSpec as P

BETA_ONE = 0.9
BETA_TWO = 0.999
ADAM_EPS = 1e-8
WEIGHT_DECAY = 0.1
ADAM_STEP = 1000


TILE = (8, 128)
TILES = 72
VMEM_LIMIT = 60 * 1024 * 1024
PART = 24
ORDERS = ((2, 1, 0), (1, 0, 2), (0, 2, 1))
HALF_PART = PART // 2
STREAMS = tuple((h, k, d) for h in (1, 0) for k in range(3) for d in range(2))
EARLY = len(STREAMS) // 2
MESH_ID = pl.DeviceIdType.MESH


def torus():
    stage = lax.axis_index("stage")
    me = lax.axis_index("data")
    coords = (me // 16, (me // 4) % 4, me % 4)
    strides = (16, 4, 1)

    def ring(axis, delta):
        return lax.rem(coords[axis] + delta + 8, 4)

    def peer(axis, delta):
        return (stage, me + (ring(axis, delta) - coords[axis]) * strides[axis])

    return stage, me, coords, ring, peer


def sgn(d):
    return 1 - 2 * d


def pick(k, on_a, on_b, on_c):
    index = [on_a] * 3
    index[ORDERS[k][1]], index[ORDERS[k][2]] = on_b, on_c
    return tuple(index)


def remote(src, dst, send_sem, recv_sem, target):
    return pltpu.make_async_remote_copy(src_ref=src, dst_ref=dst, send_sem=send_sem, recv_sem=recv_sem, device_id=target, device_id_type=MESH_ID)


def grad_view(g_ref, stream, ring, turns, i):
    h, k, d = stream
    on_a, on_b = ring(ORDERS[k][0], -sgn(d) * turns), ring(ORDERS[k][1], -sgn(d) * (1 + i))
    return g_ref.at[(h,) + pick(k, on_a, on_b, slice(None)) + (pl.ds(PART * k + HALF_PART * d, HALF_PART),)]


def tail_kernel(tau_clip, learn_rate, g_ref, early_ref, w_ref, m_ref, v_ref, loss_ref,
                w_out, m_out, v_out, stat_out, full_out,
                recv1, recv2, recv3, local, wbf, nbuf,
                s1, r1, s2, r2, s3, r3, l_sem, e_sem, own_sem, ns, nr,
                t1, q1, t2, q2, t3, q3):
    stage, me, coords, ring, peer = torus()
    streams = [(k, d) for k in range(3) for d in range(2)]

    barrier = pltpu.get_barrier_semaphore()
    for axis in range(3):
        for delta in (1, 2, 3):
            pl.semaphore_signal(barrier, inc=1, device_id=peer(axis, delta), device_id_type=MESH_ID)
    pl.semaphore_signal(barrier, inc=1, device_id=(1 - stage, me), device_id_type=MESH_ID)
    pl.semaphore_wait(barrier, 10)

    def next_of(st, phase):
        h, k, d = STREAMS[st]
        return peer(ORDERS[k][phase], sgn(d))

    def back_of(st, phase, turns):
        h, k, d = STREAMS[st]
        return ring(ORDERS[k][phase], -sgn(d) * turns)

    def first_send(st, i):
        return remote(grad_view(g_ref, STREAMS[st], ring, 1, i), recv1.at[st, 0, i], s1.at[st, 0, i], r1.at[st, 0, i], next_of(st, 0))

    def first_load(st, i):
        return pltpu.make_async_copy(early_ref.at[st, i], recv1.at[st, 0, i], e_sem.at[st, i])

    def forward1(st, step, i):
        return remote(recv1.at[st, step, i], recv1.at[st, step + 1, i], s1.at[st, step + 1, i], r1.at[st, step + 1, i], next_of(st, 0))

    def arrived1(st, step, i):
        return remote(recv1.at[st, step, i], recv1.at[st, step, i], s1.at[st, step, i], r1.at[st, step, i], next_of(st, 0))

    def fetch(st, n):
        return pltpu.make_async_copy(grad_view(g_ref, STREAMS[st], ring, 2 + n // 4, n % 4), local.at[st, n % 2], l_sem.at[st, n % 2])

    def send2(st, step):
        src = recv1.at[st, 2, 0] if step == 0 else recv2.at[st, step - 1]
        return remote(src, recv2.at[st, step], s2.at[st, step], r2.at[st, step], next_of(st, 1))

    def send3(st, step):
        src = recv2.at[st, 2, back_of(st, 2, 1)] if step == 0 else recv3.at[st, step - 1]
        return remote(src, recv3.at[st, step], s3.at[st, step], r3.at[st, step], next_of(st, 2))

    all_st = range(len(STREAMS))
    early, late = all_st[:EARLY], all_st[EARLY:]
    for i in range(4):
        for st in early:
            first_load(st, i).start()
        for st in late:
            first_send(st, i).start()
        if i == 0:
            for st in all_st:
                for n in range(2):
                    fetch(st, n).start()

    def accumulate(st, step, i, more):
        n = step * 4 + i
        if step == 0 and st < EARLY:
            first_load(st, i).wait()
        else:
            arrived1(st, step, i).wait_recv()
        fetch(st, n).wait()
        recv1[st, step, i] = recv1[st, step, i] + local[st, n % 2]
        if more:
            fetch(st, n + 2).start()

    for step in range(2):
        def phase1(i, carry):
            for st in all_st:
                accumulate(st, step, i, True)
                forward1(st, step, i).start()
            return carry

        lax.fori_loop(0, 4, phase1, 0)
    for i in range(4):
        for st in all_st:
            accumulate(st, 2, i, i < 2)
            if i == 0:
                send2(st, 0).start()
        if i > 0:
            for st in all_st:
                send2(st, i - 1).wait_recv()
                recv2[st, i - 1] = recv2[st, i - 1] + recv1[st, 2, i]
                if i < 3:
                    send2(st, i).start()
                else:
                    send3(st, 0).start()
    for step in range(3):
        for st in all_st:
            send3(st, step).wait_recv()
            recv3[st, step] = recv3[st, step] + recv2[st, 2, back_of(st, 2, 2 + step)]
            if step < 2:
                send3(st, step + 1).start()

    total = jnp.zeros((8, 128), jnp.float32)
    for st in all_st:
        piece = recv3[st, 2]
        total = total + jnp.sum(piece * piece, axis=0)

    parts = (total, loss_ref[...])
    for phase in range(4):
        size = 2 if phase == 0 else 4
        mine = stage if phase == 0 else coords[phase - 1]
        nbuf[phase, mine, 0] = parts[0]
        nbuf[phase, mine, 1] = parts[1]
        sends = []
        for delta in range(1, size):
            target = (1 - stage, me) if phase == 0 else peer(phase - 1, delta)
            sends.append(remote(nbuf.at[phase, mine], nbuf.at[phase, mine], ns.at[phase, delta], nr.at[phase, delta], target))
        for send in sends:
            send.start()
        for send in sends:
            send.wait_recv()
        parts = tuple(sum((nbuf[phase, slot, j] for slot in range(1, size)), nbuf[phase, 0, j]) for j in range(2))
        for send in sends:
            send.wait_send()

    stat_out[...] = jnp.full((8, 128), jnp.sum(parts[1]), jnp.float32)
    norm = jnp.sqrt(jnp.full((8, 128), jnp.sum(parts[0]), jnp.float32))
    clip = jnp.minimum(1.0, tau_clip / norm)

    def update(width):
        def group(k, carry):
            for h in range(2):
                for t in range(PART):
                    rows = pl.ds(k * 192 + (t // width) * (8 * width) + t % width, 8, stride=width)
                    grad = clip * recv3[(1 - h) * EARLY + 2 * k + t // HALF_PART, 2, t % HALF_PART]
                    m_new = BETA_ONE * m_ref[h, rows, :] + (1.0 - BETA_ONE) * grad
                    v_new = BETA_TWO * v_ref[h, rows, :] + (1.0 - BETA_TWO) * grad * grad
                    m_hat = m_new / (1.0 - BETA_ONE ** ADAM_STEP)
                    v_hat = v_new / (1.0 - BETA_TWO ** ADAM_STEP)
                    w_old = w_ref[h, rows, :]
                    w_new = w_old - learn_rate * (m_hat / (jnp.sqrt(v_hat) + ADAM_EPS) + WEIGHT_DECAY * w_old)
                    w_out[h, rows, :] = w_new
                    m_out[h, rows, :] = m_new
                    v_out[h, rows, :] = v_new
                    wbf[h, k * PART + t] = w_new.astype(jnp.bfloat16)
            return carry

        lax.fori_loop(0, 3, group, 0)

    @pl.when(me < 32)
    def _():
        update(24)

    @pl.when(me >= 32)
    def _():
        update(6)

    def full_part(st, on_a, on_b, on_c):
        k, d = streams[st]
        return full_out.at[(d,) + pick(k, on_a, on_b, on_c) + (pl.ds(PART * k, PART),)]

    def along(st, phase):
        k, d = streams[st]
        return peer(ORDERS[k][phase], sgn(d))

    def coord_of(st, phase, delta):
        k, d = streams[st]
        return ring(ORDERS[k][phase], -sgn(d) * delta)

    def gather1(st, step):
        k, d = streams[st]
        place = full_part(st, coord_of(st, 0, 0), coord_of(st, 1, 0), coord_of(st, 2, step))
        src = wbf.at[d, pl.ds(PART * k, PART)] if step == 0 else place
        return remote(src, place, t1.at[st, step], q1.at[st, step], along(st, 2))

    def gather2(st, step):
        place = full_part(st, coord_of(st, 0, 0), coord_of(st, 1, step), slice(None))
        return remote(place, place, t2.at[st, step], q2.at[st, step], along(st, 1))

    def gather3(st, step, i):
        place = full_part(st, coord_of(st, 0, step), coord_of(st, 1, i), slice(None))
        return remote(place, place, t3.at[st, step, i], q3.at[st, step, i], along(st, 0))

    def own(st):
        k, d = streams[st]
        return pltpu.make_async_copy(wbf.at[d, pl.ds(PART * k, PART)], full_part(st, coord_of(st, 0, 0), coord_of(st, 1, 0), coord_of(st, 2, 0)), own_sem.at[st])

    for st in range(6):
        gather1(st, 0).start()
        own(st).start()
    for step in range(3):
        for st in range(6):
            gather1(st, step).wait_recv()
            if step < 2:
                gather1(st, step + 1).start()
    for st in range(6):
        own(st).wait()
        gather2(st, 0).start()
        gather3(st, 0, 0).start()
    for step in range(3):
        for st in range(6):
            gather2(st, step).wait_recv()
            if step < 2:
                gather2(st, step + 1).start()
            gather3(st, 0, step + 1).start()

    def phase3(n, carry):
        step, i = n // 4, n % 4
        for st in range(6):
            gather3(st, step, i).wait_recv()
            gather3(st, step + 1, i).start()
        return carry

    lax.fori_loop(0, 8, phase3, 0)
    for i in range(4):
        for st in range(6):
            gather3(st, 2, i).wait_recv()

    def drain(i, carry):
        for step in range(3):
            for st in all_st:
                if step > 0 or st >= EARLY:
                    arrived1(st, step, i).wait_send()
            for st in range(6):
                gather3(st, step, i).wait_send()
        return carry

    lax.fori_loop(0, 4, drain, 0)
    for step in range(3):
        for st in all_st:
            send2(st, step).wait_send()
            send3(st, step).wait_send()
        for st in range(6):
            gather1(st, step).wait_send()
            gather2(st, step).wait_send()


def tail(grads, early, w_flat, m_flat, v_flat, loss_tile, tau_clip, learn_rate):
    f32, bf16 = jnp.float32, jnp.bfloat16
    flat = jax.ShapeDtypeStruct(w_flat.shape, f32)
    in_vmem = pl.BlockSpec(memory_space=pltpu.VMEM)
    in_any = pl.BlockSpec(memory_space=pl.ANY)
    dma = pltpu.SemaphoreType.DMA
    n_stream = len(STREAMS)
    per_step = (n_stream, 3)
    per_sub = per_step + (4,)
    part = (HALF_PART,) + TILE
    per_place = (6, 3)
    return pl.pallas_call(
        functools.partial(tail_kernel, tau_clip, learn_rate),
        out_shape=(flat, flat, flat, jax.ShapeDtypeStruct(TILE, f32), jax.ShapeDtypeStruct(grads.shape, bf16)),
        in_specs=[in_any] * 2 + [in_vmem] * 4,
        out_specs=(in_vmem, in_vmem, in_vmem, in_vmem, in_any),
        scratch_shapes=[
            pltpu.VMEM(per_sub + (4,) + part, f32),
            pltpu.VMEM(per_sub + part, f32),
            pltpu.VMEM(per_step + part, f32),
            pltpu.VMEM((n_stream, 2, 4) + part, f32),
            pltpu.VMEM((2, TILES) + TILE, bf16),
            pltpu.VMEM((4, 4, 2) + TILE, f32),
            *[dma(per_sub)] * 2, *[dma(per_step)] * 4,
            dma((n_stream, 2)), dma((EARLY, 4)), dma((6,)), *[dma((4, 4))] * 2,
            *[dma(per_place)] * 4, *[dma(per_place + (4,))] * 2,
        ],
        compiler_params=pltpu.CompilerParams(collective_id=1, has_side_effects=True, vmem_limit_bytes=VMEM_LIMIT),
        name="tail",
    )(grads, early, w_flat, m_flat, v_flat, loss_tile)


ROWS = 256
GELU_K = math.sqrt(2.0 / math.pi)
GELU_C = 0.044715


def gelu_tanh(pre, square):
    return jnp.tanh(pre * (GELU_K + (GELU_K * GELU_C) * square))


def stack_kernel(n_tokens, x_hbm, t_hbm, w1_hbm, w2_hbm, g_out, early_out, loss_out,
                 w1, w2, xs, gs, us, acts, rs, outf, outb, tgt, xt, stage1, stage2,
                 w1_sem, w2_sem, x_sem, t_sem, xsend, xrecv, gsend, grecv, o1_sem, o2_sem, es, er):
    stage, me, coords, ring, peer = torus()
    partner = (1 - stage, me)
    n_half, d_model, d_ff = w1.shape

    def load_w1(h):
        return pltpu.make_async_copy(w1_hbm.at[h], w1.at[h], w1_sem.at[h])

    def load_w2(h):
        return pltpu.make_async_copy(w2_hbm.at[h], w2.at[h], w2_sem.at[h])

    load_x = pltpu.make_async_copy(x_hbm, xs.at[0], x_sem)
    load_t = pltpu.make_async_copy(t_hbm, tgt, t_sem)

    @pl.when(stage == 0)
    def _():
        load_x.start()

    load_w1(0).start()
    load_w2(0).start()
    load_w1(1).start()
    load_w2(1).start()
    load_t.start()

    barrier = pltpu.get_barrier_semaphore()
    pl.semaphore_signal(barrier, inc=1, device_id=partner, device_id_type=MESH_ID)
    for axis in range(3):
        for d in range(2):
            pl.semaphore_signal(barrier, inc=1, device_id=peer(axis, sgn(d)), device_id_type=MESH_ID)
    pl.semaphore_wait(barrier, 7)

    @pl.when(stage == 0)
    def _():
        load_x.wait()

    loss_out[...] = jnp.zeros((8, 128), jnp.float32)

    def dot(lhs, rhs, on_left, on_right):
        return lax.dot_general(lhs, rhs, (((on_left,), (on_right,)), ((), ())), preferred_element_type=jnp.float32)

    def rows_of(c):
        return pl.ds(pl.multiple_of(c * ROWS, ROWS), ROWS)

    def block(i, size):
        return pl.ds(pl.multiple_of(i * size, size), size)

    def send_x(h, c):
        return pltpu.make_async_remote_copy(src_ref=outf.at[h, c], dst_ref=xs.at[h + stage, rows_of(c)], send_sem=xsend.at[h, c], recv_sem=xrecv.at[h + stage, c], device_id=partner, device_id_type=MESH_ID)

    def wait_x(h, c):
        pltpu.make_async_remote_copy(src_ref=outf.at[h, c], dst_ref=xs.at[h, rows_of(c)], send_sem=xsend.at[h, c], recv_sem=xrecv.at[h, c], device_id=partner, device_id_type=MESH_ID).wait_recv()

    def send_g(h, c):
        to = h - 1 + stage
        return pltpu.make_async_remote_copy(src_ref=outb.at[h, c], dst_ref=gs.at[to, rows_of(c)], send_sem=gsend.at[h, c], recv_sem=grecv.at[to, c], device_id=partner, device_id_type=MESH_ID)

    def wait_g(h, c):
        pltpu.make_async_remote_copy(src_ref=outb.at[h, c], dst_ref=gs.at[h, rows_of(c)], send_sem=gsend.at[h, c], recv_sem=grecv.at[h, c], device_id=partner, device_id_type=MESH_ID).wait_recv()

    def forward(item, carry):
        h, c = item // 2, item % 2
        rows = rows_of(c)

        @pl.when(c == 0)
        def _():
            load_w1(h).wait()

        @pl.when(h + stage > 0)
        def _():
            wait_x(h, c)

        def up(f, inner):
            cols = block(f, 512)
            pre = dot(xs[h, rows, :], w1[h, :, cols], 1, 0)
            us[h, rows, cols] = pre
            half = 0.5 * pre
            acts[h, rows, cols] = (half + half * gelu_tanh(pre, pre * pre)).astype(jnp.bfloat16)
            return inner

        lax.fori_loop(0, d_ff // 512, up, 0, unroll=True)

        @pl.when(c == 0)
        def _():
            load_w2(h).wait()

        def down(n, inner):
            cols = block(n, 256)
            val = dot(acts[h, rows, :], w2[h, :, cols], 1, 0)
            outf[h, c, :, cols] = (xs[h, rows, cols].astype(jnp.float32) + val).astype(jnp.bfloat16)
            return inner

        lax.fori_loop(0, d_model // 256, down, 0)

        @pl.when(h + stage < 2)
        def _():
            send_x(h, c).start()

        @pl.when(h + stage == 2)
        def _():
            @pl.when(c == 0)
            def _():
                load_t.wait()

            residual = outf[h, c].astype(jnp.float32) - tgt[rows, :].astype(jnp.float32)
            gs[h, rows, :] = (residual / n_tokens).astype(jnp.bfloat16)
            square = residual * residual
            part = sum(square[:, 128 * j:128 * (j + 1)] for j in range(d_model // 128))
            loss_out[...] += 0.5 * jnp.sum(part.reshape(ROWS // 8, 8, 128), axis=0)

        return carry

    lax.fori_loop(0, 2 * n_half, forward, 0)

    @pl.when(stage == 0)
    def _():
        load_t.wait()

    def out_one(h, n, i):
        return pltpu.make_async_copy(stage1.at[n % 2, i], g_out.at[h, pl.ds(0, 2), :, :, pl.ds(i * 24 + 2 * n, 2)], o1_sem.at[n % 2, i])

    def out_two(h, m):
        return pltpu.make_async_copy(stage2.at[m % 2], g_out.at[h, 2 + m // 4, m % 4], o2_sem.at[m % 2])

    def early_send(st, i):
        h, k, d = STREAMS[st]
        return remote(grad_view(g_out, STREAMS[st], ring, 1, i), early_out.at[st, i], es.at[st, i], er.at[st, i], peer(ORDERS[k][0], sgn(d)))

    def backward(b, carry):
        h = 1 - b

        def chain(c, inner):
            rows = rows_of(c)

            @pl.when(h + stage < 2)
            def _():
                wait_g(h, c)

            def up(f, deep):
                cols = block(f, 512)
                q = dot(gs[h, rows, :], w2[h, cols, :], 1, 1)
                pre = us[h, rows, cols]
                square = pre * pre
                th = gelu_tanh(pre, square)
                slope = (0.5 + 0.5 * th) + (1.0 - th * th) * (pre * (0.5 * GELU_K + (1.5 * GELU_K * GELU_C) * square))
                rs[rows, cols] = (q * slope).astype(jnp.bfloat16)
                return deep

            lax.fori_loop(0, d_ff // 512, up, 0, unroll=True)

            @pl.when(h + stage > 0)
            def _():
                def down(n, deep):
                    cols = block(n, 256)
                    val = dot(rs[rows, :], w1[h, cols, :], 1, 1)
                    outb[h, c, :, cols] = (gs[h, rows, cols].astype(jnp.float32) + val).astype(jnp.bfloat16)
                    return deep

                lax.fori_loop(0, d_model // 256, down, 0)
                send_g(h, c).start()

            return inner

        lax.fori_loop(0, 2, chain, 0)

        xt[...] = xs[h].T

        def grad_one(n, inner):
            @pl.when(n >= 2)
            def _():
                for i in range(3):
                    out_one(h, n, i).wait()

            val = dot(xt[...], rs[:, block(n, 256)], 1, 0)
            for p in range(32):
                for i in range(3):
                    for j in range(2):
                        stage1[n % 2, i, p // 16, (p // 4) % 4, p % 4, j] = val[p * 24 + i * 8:p * 24 + i * 8 + 8, 128 * j:128 * (j + 1)]
            for i in range(3):
                out_one(h, n, i).start()
            return inner

        lax.fori_loop(0, d_ff // 256, grad_one, 0)

        def grad_two(m, inner):
            @pl.when(m >= 2)
            def _():
                out_two(h, m).wait()

            val = dot(acts[h, :, block(m, 384)], gs[h], 0, 0)
            for p in range(4):
                for i in range(12):
                    for j in range(6):
                        stage2[m % 2, p, i * 6 + j] = val[p * 96 + i * 8:p * 96 + i * 8 + 8, 128 * j:128 * (j + 1)]
            out_two(h, m).start()
            return inner

        lax.fori_loop(0, d_ff // 384, grad_two, 0)
        for n in range(2):
            for i in range(3):
                out_one(h, n, i).wait()
            out_two(h, n).wait()

        @pl.when(b == 0)
        def _():
            for i in range(4):
                for st in range(EARLY):
                    early_send(st, i).start()

        return carry

    lax.fori_loop(0, n_half, backward, 0)
    for i in range(4):
        for st in range(EARLY):
            early_send(st, i).wait()

    for h in range(2):
        for c in range(2):
            @pl.when(h + stage < 2)
            def _():
                send_x(h, c).wait_send()

            @pl.when(h + stage > 0)
            def _():
                send_g(h, c).wait_send()


def stack(x_all, t_all, w1, w2, n_tokens):
    rows, d_model = x_all.shape
    d_ff = w1.shape[2]
    bf16, f32 = jnp.bfloat16, jnp.float32
    dma = pltpu.SemaphoreType.DMA
    in_any = pl.BlockSpec(memory_space=pl.ANY)
    return pl.pallas_call(
        functools.partial(stack_kernel, n_tokens),
        out_shape=(jax.ShapeDtypeStruct((2, 4, 4, 4, TILES) + TILE, f32), jax.ShapeDtypeStruct((EARLY, 4, 4, HALF_PART) + TILE, f32), jax.ShapeDtypeStruct(TILE, f32)),
        in_specs=[in_any] * 4,
        out_specs=(in_any, in_any, pl.BlockSpec(memory_space=pltpu.VMEM)),
        scratch_shapes=[
            pltpu.VMEM((2, d_model, d_ff), bf16), pltpu.VMEM((2, d_ff, d_model), bf16),
            pltpu.VMEM((2, rows, d_model), bf16), pltpu.VMEM((2, rows, d_model), bf16),
            pltpu.VMEM((2, rows, d_ff), f32), pltpu.VMEM((2, rows, d_ff), bf16), pltpu.VMEM((rows, d_ff), bf16),
            pltpu.VMEM((2, 2, ROWS, d_model), bf16), pltpu.VMEM((2, 2, ROWS, d_model), bf16), pltpu.VMEM((rows, d_model), bf16), pltpu.VMEM((d_model, rows), bf16),
            pltpu.VMEM((2, 3, 2, 4, 4, 2) + TILE, f32), pltpu.VMEM((2, 4, TILES) + TILE, f32),
            dma((2,)), dma((2,)), dma, dma, *[dma((2, 2))] * 4, dma((2, 3)), dma((2,)), *[dma((EARLY, 4))] * 2,
        ],
        compiler_params=pltpu.CompilerParams(collective_id=0, has_side_effects=True, vmem_limit_bytes=VMEM_LIMIT),
        name="stack",
    )(x_all, t_all, w1, w2)


def solution(mesh):
    n_stage = mesh.shape["stage"]
    n_data = mesh.shape["data"]

    def device_step(x_loc, t_loc, w1_loc, w2_loc, wm_loc, m_loc, v_loc):
        n_micro, n_tok, d_model = x_loc.shape
        d_ff = w1_loc.shape[4]
        n_tokens = n_micro * n_tok * n_data
        n_blocks = 2 * n_stage
        tau_clip = 0.3 * d_model * math.sqrt(n_blocks * (3.0 / n_tokens + 0.008))
        learn_rate = 0.1 / math.sqrt(4.0 * d_model * n_blocks)
        x_all = x_loc.reshape(n_micro * n_tok, d_model)
        t_all = t_loc.reshape(n_micro * n_tok, d_model)
        grads, early, loss_tile = stack(x_all, t_all, w1_loc[0, :, 0], w2_loc[0, :, 0], n_tokens)
        w_new, m_new, v_new, stat, w_full = tail(
            grads, early, wm_loc.reshape(2, 576, 128), m_loc.reshape(2, 576, 128), v_loc.reshape(2, 576, 128),
            loss_tile, tau_clip, learn_rate)
        w1_new = w_full[:, :2].reshape(2, d_model // 8, d_ff // 128, 8, 128).transpose(0, 1, 3, 2, 4).reshape(1, 2, 1, d_model, d_ff)
        w2_new = w_full[:, 2:].reshape(2, d_ff // 8, d_model // 128, 8, 128).transpose(0, 1, 3, 2, 4).reshape(1, 2, 1, d_ff, d_model)
        flat_dims = (1, 2, 1, -1)
        return w1_new, w2_new, w_new.reshape(flat_dims), m_new.reshape(flat_dims), v_new.reshape(flat_dims), stat[0, 0] / n_tokens

    act_spec = P(None, "data", None)
    flat_spec = P("stage", None, None, "data")
    return jax.shard_map(device_step, mesh=mesh, in_specs=(act_spec, act_spec, P("stage"), P("stage"), flat_spec, flat_spec, flat_spec), out_specs=(P("stage"), P("stage"), flat_spec, flat_spec, flat_spec, P()), check_vma=False)
```

```python
import functools
import math
import jax
import jax.numpy as jnp
from jax import lax
from jax.experimental import pallas as pl
from jax.experimental.pallas import tpu as pltpu
from jax.sharding import PartitionSpec as P

BETA_ONE = 0.9
BETA_TWO = 0.999
ADAM_EPS = 1e-8
WEIGHT_DECAY = 0.1
ADAM_STEP = 1000


TILE = (8, 128)
TILES = 72
VMEM_LIMIT = 60 * 1024 * 1024
PART = 24
ORDERS = ((2, 1, 0), (1, 0, 2), (0, 2, 1))
HALF_PART = PART // 2
STREAMS = tuple((h, k, d) for h in (1, 0) for k in range(3) for d in range(2))
EARLY = len(STREAMS) // 2
MESH_ID = pl.DeviceIdType.MESH


def torus():
    stage = lax.axis_index("stage")
    me = lax.axis_index("data")
    coords = (me // 16, (me // 4) % 4, me % 4)
    strides = (16, 4, 1)

    def ring(axis, delta):
        return lax.rem(coords[axis] + delta + 8, 4)

    def peer(axis, delta):
        return (stage, me + (ring(axis, delta) - coords[axis]) * strides[axis])

    return stage, me, coords, ring, peer


def sgn(d):
    return 1 - 2 * d


def pick(k, on_a, on_b, on_c):
    index = [on_a] * 3
    index[ORDERS[k][1]], index[ORDERS[k][2]] = on_b, on_c
    return tuple(index)


def remote(src, dst, send_sem, recv_sem, target):
    return pltpu.make_async_remote_copy(src_ref=src, dst_ref=dst, send_sem=send_sem, recv_sem=recv_sem, device_id=target, device_id_type=MESH_ID)


def grad_view(g_ref, stream, ring, turns, i):
    h, k, d = stream
    on_a, on_b = ring(ORDERS[k][0], -sgn(d) * turns), ring(ORDERS[k][1], -sgn(d) * (1 + i))
    return g_ref.at[(h,) + pick(k, on_a, on_b, slice(None)) + (pl.ds(PART * k + HALF_PART * d, HALF_PART),)]


def tail_kernel(tau_clip, learn_rate, g_ref, early_ref, w_ref, m_ref, v_ref, loss_ref,
                w_out, m_out, v_out, stat_out, full_out,
                recv1, recv2, recv3, local, wbf, nbuf, state,
                s1, r1, s2, r2, s3, r3, l_sem, e_sem, own_sem, ns, nr, in_sem, out_sem,
                t1, q1, t2, q2, t3, q3):
    stage, me, coords, ring, peer = torus()
    streams = [(k, d) for k in range(3) for d in range(2)]

    barrier = pltpu.get_barrier_semaphore()
    for axis in range(3):
        for delta in (1, 2, 3):
            pl.semaphore_signal(barrier, inc=1, device_id=peer(axis, delta), device_id_type=MESH_ID)
    pl.semaphore_signal(barrier, inc=1, device_id=(1 - stage, me), device_id_type=MESH_ID)
    pl.semaphore_wait(barrier, 10)

    def next_of(st, phase):
        h, k, d = STREAMS[st]
        return peer(ORDERS[k][phase], sgn(d))

    def back_of(st, phase, turns):
        h, k, d = STREAMS[st]
        return ring(ORDERS[k][phase], -sgn(d) * turns)

    def first_send(st, i):
        return remote(grad_view(g_ref, STREAMS[st], ring, 1, i), recv1.at[st, 0, i], s1.at[st, 0, i], r1.at[st, 0, i], next_of(st, 0))

    def first_load(st, i):
        return pltpu.make_async_copy(early_ref.at[st, i], recv1.at[st, 0, i], e_sem.at[st, i])

    def forward1(st, step, i):
        return remote(recv1.at[st, step, i], recv1.at[st, step + 1, i], s1.at[st, step + 1, i], r1.at[st, step + 1, i], next_of(st, 0))

    def arrived1(st, step, i):
        return remote(recv1.at[st, step, i], recv1.at[st, step, i], s1.at[st, step, i], r1.at[st, step, i], next_of(st, 0))

    def fetch(st, n):
        return pltpu.make_async_copy(grad_view(g_ref, STREAMS[st], ring, 2 + n // 4, n % 4), local.at[st, n % 2], l_sem.at[st, n % 2])

    def send2(st, step):
        src = recv1.at[st, 2, 0] if step == 0 else recv2.at[st, step - 1]
        return remote(src, recv2.at[st, step], s2.at[st, step], r2.at[st, step], next_of(st, 1))

    def send3(st, step):
        src = recv2.at[st, 2, back_of(st, 2, 1)] if step == 0 else recv3.at[st, step - 1]
        return remote(src, recv3.at[st, step], s3.at[st, step], r3.at[st, step], next_of(st, 2))

    state_in = [pltpu.make_async_copy(ref, state.at[j], in_sem.at[j]) for j, ref in enumerate((w_ref, m_ref, v_ref))]
    state_out = [pltpu.make_async_copy(state.at[j], ref, out_sem.at[j]) for j, ref in enumerate((w_out, m_out, v_out))]
    all_st = range(len(STREAMS))
    early, late = all_st[:EARLY], all_st[EARLY:]
    for i in range(4):
        for st in early:
            first_load(st, i).start()
        for st in late:
            first_send(st, i).start()
        if i == 0:
            for st in all_st:
                for n in range(2):
                    fetch(st, n).start()

    for copy in state_in:
        copy.start()

    def accumulate(st, step, i, more):
        n = step * 4 + i
        if step == 0 and st < EARLY:
            first_load(st, i).wait()
        else:
            arrived1(st, step, i).wait_recv()
        fetch(st, n).wait()
        recv1[st, step, i] = recv1[st, step, i] + local[st, n % 2]
        if more:
            fetch(st, n + 2).start()

    for step in range(2):
        def phase1(i, carry):
            for st in all_st:
                accumulate(st, step, i, True)
                forward1(st, step, i).start()
            return carry

        lax.fori_loop(0, 4, phase1, 0)
    for i in range(4):
        for st in all_st:
            accumulate(st, 2, i, i < 2)
            if i == 0:
                send2(st, 0).start()
        if i > 0:
            for st in all_st:
                send2(st, i - 1).wait_recv()
                recv2[st, i - 1] = recv2[st, i - 1] + recv1[st, 2, i]
                if i < 3:
                    send2(st, i).start()
                else:
                    send3(st, 0).start()
    for step in range(3):
        for st in all_st:
            send3(st, step).wait_recv()
            recv3[st, step] = recv3[st, step] + recv2[st, 2, back_of(st, 2, 2 + step)]
            if step < 2:
                send3(st, step + 1).start()

    for copy in state_in:
        copy.wait()
    total = jnp.zeros(TILE, jnp.float32)
    for st in all_st:
        piece = recv3[st, 2]
        total = total + jnp.sum(piece * piece, axis=0)

    parts = (total, loss_ref[...])
    for phase in range(4):
        size = 2 if phase == 0 else 4
        mine = stage if phase == 0 else coords[phase - 1]
        nbuf[phase, mine, 0] = parts[0]
        nbuf[phase, mine, 1] = parts[1]
        sends = []
        for delta in range(1, size):
            target = (1 - stage, me) if phase == 0 else peer(phase - 1, delta)
            sends.append(remote(nbuf.at[phase, mine], nbuf.at[phase, mine], ns.at[phase, delta], nr.at[phase, delta], target))
        for send in sends:
            send.start()
        for send in sends:
            send.wait_recv()
        parts = tuple(sum((nbuf[phase, slot, j] for slot in range(1, size)), nbuf[phase, 0, j]) for j in range(2))
        for send in sends:
            send.wait_send()

    stat_out[...] = jnp.full((8, 128), jnp.sum(parts[1]), jnp.float32)
    norm = jnp.sqrt(jnp.full((8, 128), jnp.sum(parts[0]), jnp.float32))
    clip = jnp.minimum(1.0, tau_clip / norm)

    def update(width):
        def group(k, carry):
            for h in range(2):
                for t in range(PART):
                    rows = pl.ds(k * 192 + (t // width) * (8 * width) + t % width, 8, stride=width)
                    grad = clip * recv3[(1 - h) * EARLY + 2 * k + t // HALF_PART, 2, t % HALF_PART]
                    m_new = BETA_ONE * state[1, h, rows, :] + (1.0 - BETA_ONE) * grad
                    v_new = BETA_TWO * state[2, h, rows, :] + (1.0 - BETA_TWO) * grad * grad
                    m_hat = m_new * (1.0 / (1.0 - BETA_ONE ** ADAM_STEP))
                    v_hat = v_new * (1.0 / (1.0 - BETA_TWO ** ADAM_STEP))
                    w_old = state[0, h, rows, :]
                    w_new = w_old - learn_rate * (m_hat / (jnp.sqrt(v_hat) + ADAM_EPS) + WEIGHT_DECAY * w_old)
                    state[0, h, rows, :] = w_new
                    state[1, h, rows, :] = m_new
                    state[2, h, rows, :] = v_new
                    wbf[h, k * PART + t] = w_new.astype(jnp.bfloat16)
            return carry

        lax.fori_loop(0, 3, group, 0)

    @pl.when(me < 32)
    def _():
        update(24)

    @pl.when(me >= 32)
    def _():
        update(6)

    for copy in state_out:
        copy.start()

    def full_part(st, on_a, on_b, on_c):
        k, d = streams[st]
        return full_out.at[(d,) + pick(k, on_a, on_b, on_c) + (pl.ds(PART * k, PART),)]

    def along(st, phase):
        k, d = streams[st]
        return peer(ORDERS[k][phase], sgn(d))

    def coord_of(st, phase, delta):
        k, d = streams[st]
        return ring(ORDERS[k][phase], -sgn(d) * delta)

    def gather1(st, step):
        k, d = streams[st]
        place = full_part(st, coord_of(st, 0, 0), coord_of(st, 1, 0), coord_of(st, 2, step))
        src = wbf.at[d, pl.ds(PART * k, PART)] if step == 0 else place
        return remote(src, place, t1.at[st, step], q1.at[st, step], along(st, 2))

    def gather2(st, step):
        place = full_part(st, coord_of(st, 0, 0), coord_of(st, 1, step), slice(None))
        return remote(place, place, t2.at[st, step], q2.at[st, step], along(st, 1))

    def gather3(st, step, i):
        place = full_part(st, coord_of(st, 0, step), coord_of(st, 1, i), slice(None))
        return remote(place, place, t3.at[st, step, i], q3.at[st, step, i], along(st, 0))

    def own(st):
        k, d = streams[st]
        return pltpu.make_async_copy(wbf.at[d, pl.ds(PART * k, PART)], full_part(st, coord_of(st, 0, 0), coord_of(st, 1, 0), coord_of(st, 2, 0)), own_sem.at[st])

    for st in range(6):
        gather1(st, 0).start()
        own(st).start()
    for step in range(3):
        for st in range(6):
            gather1(st, step).wait_recv()
            if step < 2:
                gather1(st, step + 1).start()
    for st in range(6):
        own(st).wait()
        gather2(st, 0).start()
        gather3(st, 0, 0).start()
    for step in range(3):
        for st in range(6):
            gather2(st, step).wait_recv()
            if step < 2:
                gather2(st, step + 1).start()
            gather3(st, 0, step + 1).start()

    def phase3(n, carry):
        step, i = n // 4, n % 4
        for st in range(6):
            gather3(st, step, i).wait_recv()
            gather3(st, step + 1, i).start()
        return carry

    lax.fori_loop(0, 8, phase3, 0)
    for i in range(4):
        for st in range(6):
            gather3(st, 2, i).wait_recv()

    def drain(i, carry):
        for step in range(3):
            for st in all_st:
                if step > 0 or st >= EARLY:
                    arrived1(st, step, i).wait_send()
            for st in range(6):
                gather3(st, step, i).wait_send()
        return carry

    lax.fori_loop(0, 4, drain, 0)
    for copy in state_out:
        copy.wait()
    for step in range(3):
        for st in all_st:
            send2(st, step).wait_send()
            send3(st, step).wait_send()
        for st in range(6):
            gather1(st, step).wait_send()
            gather2(st, step).wait_send()


def tail(grads, early, w_flat, m_flat, v_flat, loss_tile, tau_clip, learn_rate):
    f32, bf16 = jnp.float32, jnp.bfloat16
    flat = jax.ShapeDtypeStruct(w_flat.shape, f32)
    in_vmem = pl.BlockSpec(memory_space=pltpu.VMEM)
    in_any = pl.BlockSpec(memory_space=pl.ANY)
    dma = pltpu.SemaphoreType.DMA
    n_stream = len(STREAMS)
    per_step = (n_stream, 3)
    per_sub = per_step + (4,)
    part = (HALF_PART,) + TILE
    per_place = (6, 3)
    return pl.pallas_call(
        functools.partial(tail_kernel, tau_clip, learn_rate),
        out_shape=(flat, flat, flat, jax.ShapeDtypeStruct(TILE, f32), jax.ShapeDtypeStruct(grads.shape, bf16)),
        in_specs=[in_any] * 5 + [in_vmem],
        out_specs=(in_any, in_any, in_any, in_vmem, in_any),
        scratch_shapes=[
            pltpu.VMEM(per_sub + (4,) + part, f32),
            pltpu.VMEM(per_sub + part, f32),
            pltpu.VMEM(per_step + part, f32),
            pltpu.VMEM((n_stream, 2, 4) + part, f32),
            pltpu.VMEM((2, TILES) + TILE, bf16),
            pltpu.VMEM((4, 4, 2) + TILE, f32),
            pltpu.VMEM((3,) + w_flat.shape, f32),
            *[dma(per_sub)] * 2, *[dma(per_step)] * 4,
            dma((n_stream, 2)), dma((EARLY, 4)), dma((6,)), *[dma((4, 4))] * 2, *[dma((3,))] * 2,
            *[dma(per_place)] * 4, *[dma(per_place + (4,))] * 2,
        ],
        compiler_params=pltpu.CompilerParams(collective_id=1, has_side_effects=True, vmem_limit_bytes=VMEM_LIMIT),
        name="tail",
    )(grads, early, w_flat, m_flat, v_flat, loss_tile)


ROWS = 256
SLOTS = 4
BAND = 256
GELU_K = math.sqrt(2.0 / math.pi)
GELU_C = 0.044715


def gelu_tanh(pre, square):
    return jnp.tanh(pre * (GELU_K + (GELU_K * GELU_C) * square))


def stack_kernel(n_tokens, x_hbm, t_hbm, w1_hbm, w2_hbm, g_out, early_out, loss_out,
                 w1, w2, xs, gs, us, acts, rs, outf, outb, tgt, xt, stage1, stage2,
                 w1_sem, w2_sem, x_sem, t_sem, xsend, xrecv, gsend, grecv, o1_sem, o2_sem, es, er):
    stage, me, coords, ring, peer = torus()
    partner = (1 - stage, me)
    n_half, d_model, d_ff = w1.shape

    def load_w1(h):
        return pltpu.make_async_copy(w1_hbm.at[h], w1.at[h], w1_sem.at[h])

    def load_w2(h):
        return pltpu.make_async_copy(w2_hbm.at[h], w2.at[h], w2_sem.at[h])

    load_x = pltpu.make_async_copy(x_hbm, xs.at[0], x_sem)
    load_t = pltpu.make_async_copy(t_hbm, tgt, t_sem)

    @pl.when(stage == 0)
    def _():
        load_x.start()

    load_w1(0).start()

    barrier = pltpu.get_barrier_semaphore()
    pl.semaphore_signal(barrier, inc=1, device_id=partner, device_id_type=MESH_ID)
    for axis in range(3):
        for d in range(2):
            pl.semaphore_signal(barrier, inc=1, device_id=peer(axis, sgn(d)), device_id_type=MESH_ID)
    pl.semaphore_wait(barrier, 7)

    load_w2(0).start()

    @pl.when(stage == 0)
    def _():
        load_x.wait()

    loss_out[...] = jnp.zeros((8, 128), jnp.float32)

    def dot(lhs, rhs, on_left, on_right):
        return lax.dot_general(lhs, rhs, (((on_left,), (on_right,)), ((), ())), preferred_element_type=jnp.float32)

    def rows_of(c):
        return pl.ds(pl.multiple_of(c * ROWS, ROWS), ROWS)

    def block(i, size):
        return pl.ds(pl.multiple_of(i * size, size), size)

    def send_x(h, c, n):
        cols = block(n, BAND)
        return remote(outf.at[h, c, :, cols], xs.at[h + stage, rows_of(c), cols], xsend.at[h, c, n], xrecv.at[h + stage, c, n], partner)

    def wait_x(h, c, n):
        cols = block(n, BAND)
        remote(outf.at[h, c, :, cols], xs.at[h, rows_of(c), cols], xsend.at[h, c, n], xrecv.at[h, c, n], partner).wait_recv()

    def send_g(h, c, n):
        to, cols = h - 1 + stage, block(n, BAND)
        return remote(outb.at[h, c, :, cols], gs.at[to, rows_of(c), cols], gsend.at[h, c, n], grecv.at[to, c, n], partner)

    def wait_g(h, c, n):
        cols = block(n, BAND)
        remote(outb.at[h, c, :, cols], gs.at[h, rows_of(c), cols], gsend.at[h, c, n], grecv.at[h, c, n], partner).wait_recv()

    def forward(item, carry):
        h, c = item // 2, item % 2
        rows = rows_of(c)

        @pl.when(c == 0)
        def _():
            load_w1(h).wait()

        @pl.when(h + stage > 0)
        def _():
            for n in range(3):
                wait_x(h, c, n)

        def up(f, inner):
            cols = block(f, 512)
            pre = dot(xs[h, rows, :], w1[h, :, cols], 1, 0)
            us[h, rows, cols] = pre
            half = 0.5 * pre
            acts[h, rows, cols] = (half + half * gelu_tanh(pre, pre * pre)).astype(jnp.bfloat16)
            return inner

        lax.fori_loop(0, d_ff // 512, up, 0, unroll=True)

        @pl.when(c == 0)
        def _():
            load_w2(h).wait()

        @pl.when(item == 0)
        def _():
            load_w1(1).start()
            load_w2(1).start()
            load_t.start()

        def down(n, inner):
            cols = block(n, BAND)
            val = dot(acts[h, rows, :], w2[h, :, cols], 1, 0)
            outf[h, c, :, cols] = (xs[h, rows, cols].astype(jnp.float32) + val).astype(jnp.bfloat16)

            @pl.when(h + stage < 2)
            def _():
                send_x(h, c, n).start()

            return inner

        lax.fori_loop(0, d_model // BAND, down, 0)

        @pl.when(h + stage == 2)
        def _():
            @pl.when(c == 0)
            def _():
                load_t.wait()

            residual = outf[h, c].astype(jnp.float32) - tgt[rows, :].astype(jnp.float32)
            gs[h, rows, :] = (residual / n_tokens).astype(jnp.bfloat16)
            square = residual * residual
            part = sum(square[:, 128 * j:128 * (j + 1)] for j in range(d_model // 128))
            loss_out[...] += 0.5 * jnp.sum(part.reshape(ROWS // 8, 8, 128), axis=0)

        return carry

    lax.fori_loop(0, 2 * n_half, forward, 0)

    @pl.when(stage == 0)
    def _():
        load_t.wait()

    def out_one(h, n, i):
        return pltpu.make_async_copy(stage1.at[n % SLOTS, i], g_out.at[h, pl.ds(0, 2), :, :, pl.ds(i * 24 + 2 * n, 2)], o1_sem.at[n % SLOTS, i])

    def out_two(h, m):
        return pltpu.make_async_copy(stage2.at[m % SLOTS], g_out.at[h, 2 + m // 4, m % 4], o2_sem.at[m % SLOTS])

    def early_send(st, i):
        h, k, d = STREAMS[st]
        return remote(grad_view(g_out, STREAMS[st], ring, 1, i), early_out.at[st, i], es.at[st, i], er.at[st, i], peer(ORDERS[k][0], sgn(d)))

    def backward(b, carry):
        h = 1 - b

        def chain(c, inner):
            rows = rows_of(c)

            @pl.when(h + stage < 2)
            def _():
                for n in range(3):
                    wait_g(h, c, n)

            def up(f, deep):
                cols = block(f, 512)
                q = dot(gs[h, rows, :], w2[h, cols, :], 1, 1)
                pre = us[h, rows, cols]
                square = pre * pre
                th = gelu_tanh(pre, square)
                slope = (0.5 + 0.5 * th) + (1.0 - th * th) * (pre * (0.5 * GELU_K + (1.5 * GELU_K * GELU_C) * square))
                rs[rows, cols] = (q * slope).astype(jnp.bfloat16)
                return deep

            lax.fori_loop(0, d_ff // 512, up, 0, unroll=True)

            @pl.when(h + stage > 0)
            def _():
                def down(n, deep):
                    cols = block(n, BAND)
                    val = dot(rs[rows, :], w1[h, cols, :], 1, 1)
                    outb[h, c, :, cols] = (gs[h, rows, cols].astype(jnp.float32) + val).astype(jnp.bfloat16)
                    send_g(h, c, n).start()
                    return deep

                lax.fori_loop(0, d_model // BAND, down, 0)

            return inner

        lax.fori_loop(0, 2, chain, 0)

        xt[...] = xs[h].T

        def grad_one(n, inner):
            @pl.when(n >= SLOTS)
            def _():
                for i in range(3):
                    out_one(h, n, i).wait()

            val = dot(xt[...], rs[:, block(n, BAND)], 1, 0)
            for p in range(32):
                for i in range(3):
                    for j in range(2):
                        stage1[n % SLOTS, i, p // 16, (p // 4) % 4, p % 4, j] = val[p * 24 + i * 8:p * 24 + i * 8 + 8, 128 * j:128 * (j + 1)]
            for i in range(3):
                out_one(h, n, i).start()
            return inner

        lax.fori_loop(0, d_ff // BAND, grad_one, 0)

        def grad_two(m, inner):
            @pl.when(m >= SLOTS)
            def _():
                out_two(h, m).wait()

            val = dot(acts[h, :, block(m, 384)], gs[h], 0, 0)
            for p in range(4):
                for i in range(12):
                    for j in range(6):
                        stage2[m % SLOTS, p, i * 6 + j] = val[p * 96 + i * 8:p * 96 + i * 8 + 8, 128 * j:128 * (j + 1)]
            out_two(h, m).start()
            return inner

        lax.fori_loop(0, d_ff // 384, grad_two, 0)
        for n in range(SLOTS):
            for i in range(3):
                out_one(h, n, i).wait()
            out_two(h, n).wait()

        @pl.when(b == 0)
        def _():
            for i in range(4):
                for st in range(EARLY):
                    early_send(st, i).start()

        return carry

    lax.fori_loop(0, n_half, backward, 0)
    for i in range(4):
        for st in range(EARLY):
            early_send(st, i).wait()

    for h in range(2):
        for c in range(2):
            @pl.when(h + stage < 2)
            def _():
                for n in range(3):
                    send_x(h, c, n).wait_send()

            @pl.when(h + stage > 0)
            def _():
                for n in range(3):
                    send_g(h, c, n).wait_send()


def stack(x_all, t_all, w1, w2, n_tokens):
    rows, d_model = x_all.shape
    d_ff = w1.shape[2]
    bf16, f32 = jnp.bfloat16, jnp.float32
    dma = pltpu.SemaphoreType.DMA
    in_any = pl.BlockSpec(memory_space=pl.ANY)
    return pl.pallas_call(
        functools.partial(stack_kernel, n_tokens),
        out_shape=(jax.ShapeDtypeStruct((2, 4, 4, 4, TILES) + TILE, f32), jax.ShapeDtypeStruct((EARLY, 4, 4, HALF_PART) + TILE, f32), jax.ShapeDtypeStruct(TILE, f32)),
        in_specs=[in_any] * 4,
        out_specs=(in_any, in_any, pl.BlockSpec(memory_space=pltpu.VMEM)),
        scratch_shapes=[
            pltpu.VMEM((2, d_model, d_ff), bf16), pltpu.VMEM((2, d_ff, d_model), bf16),
            pltpu.VMEM((2, rows, d_model), bf16), pltpu.VMEM((2, rows, d_model), bf16),
            pltpu.VMEM((2, rows, d_ff), f32), pltpu.VMEM((2, rows, d_ff), bf16), pltpu.VMEM((rows, d_ff), bf16),
            pltpu.VMEM((2, 2, ROWS, d_model), bf16), pltpu.VMEM((2, 2, ROWS, d_model), bf16), pltpu.VMEM((rows, d_model), bf16), pltpu.VMEM((d_model, rows), bf16),
            pltpu.VMEM((SLOTS, 3, 2, 4, 4, 2) + TILE, f32), pltpu.VMEM((SLOTS, 4, TILES) + TILE, f32),
            dma((2,)), dma((2,)), dma, dma, *[dma((2, 2, 3))] * 4, dma((SLOTS, 3)), dma((SLOTS,)), *[dma((EARLY, 4))] * 2,
        ],
        compiler_params=pltpu.CompilerParams(collective_id=0, has_side_effects=True, vmem_limit_bytes=VMEM_LIMIT),
        name="stack",
    )(x_all, t_all, w1, w2)


def finish_kernel(full_ref, w_ref, m_ref, v_ref, stat_ref, w1_out, w2_out, w_out, m_out, v_out, loss_out, full, state, in_sem, out_sem, sin_sem, sout_sem):
    places = [(h, z, y) for h in range(2) for z in range(4) for y in range(4)]
    loads, stores = [], []
    for n, (h, z, y) in enumerate(places):
        target = w1_out if z < 2 else w2_out
        loads.append(pltpu.make_async_copy(full_ref.at[h, z, y], full.at[n], in_sem.at[n]))
        stores.append(pltpu.make_async_copy(full.at[n], target.at[h, z % 2, y], out_sem.at[n]))
    for j, (src, dst) in enumerate(((w_ref, w_out), (m_ref, m_out), (v_ref, v_out))):
        loads.append(pltpu.make_async_copy(src, state.at[j], sin_sem.at[j]))
        stores.append(pltpu.make_async_copy(state.at[j], dst, sout_sem.at[j]))
    for load in loads:
        load.start()
    for load, store in zip(loads, stores):
        load.wait()
        store.start()
    loss_out[0] = jnp.max(stat_ref[...])
    for store in stores:
        store.wait()


def finish(w_full, w_flat, m_flat, v_flat, stat):
    flat = jax.ShapeDtypeStruct(w_flat.shape, jnp.float32)
    half = jax.ShapeDtypeStruct((2, 2) + w_full.shape[2:], jnp.bfloat16)
    in_any = pl.BlockSpec(memory_space=pl.ANY)
    dma = pltpu.SemaphoreType.DMA
    return pl.pallas_call(
        finish_kernel,
        out_shape=(half, half, flat, flat, flat, jax.ShapeDtypeStruct((1,), jnp.float32)),
        in_specs=[in_any] * 4 + [pl.BlockSpec(memory_space=pltpu.VMEM)],
        out_specs=(in_any,) * 5 + (pl.BlockSpec(memory_space=pltpu.SMEM),),
        scratch_shapes=[pltpu.VMEM((32,) + w_full.shape[3:], jnp.bfloat16), pltpu.VMEM((3,) + w_flat.shape, jnp.float32), dma((32,)), dma((32,)), dma((3,)), dma((3,))],
        compiler_params=pltpu.CompilerParams(vmem_limit_bytes=VMEM_LIMIT),
        name="finish",
    )(w_full, w_flat, m_flat, v_flat, stat)


def solution(mesh):
    n_stage = mesh.shape["stage"]
    n_data = mesh.shape["data"]

    def device_step(x_loc, t_loc, w1_loc, w2_loc, wm_loc, m_loc, v_loc):
        n_micro, n_tok, d_model = x_loc.shape
        d_ff = w1_loc.shape[4]
        n_tokens = n_micro * n_tok * n_data
        n_blocks = 2 * n_stage
        tau_clip = 0.3 * d_model * math.sqrt(n_blocks * (3.0 / n_tokens + 0.008))
        learn_rate = 0.1 / math.sqrt(4.0 * d_model * n_blocks)
        x_all = x_loc.reshape(n_micro * n_tok, d_model)
        t_all = t_loc.reshape(n_micro * n_tok, d_model)
        grads, early, loss_tile = stack(x_all, t_all, w1_loc[0, :, 0], w2_loc[0, :, 0], n_tokens)
        w_new, m_new, v_new, stat, w_full = tail(
            grads, early, wm_loc.reshape(2, 576, 128), m_loc.reshape(2, 576, 128), v_loc.reshape(2, 576, 128),
            loss_tile, tau_clip, learn_rate)
        w1_new, w2_new, w_new, m_new, v_new, loss = finish(w_full, w_new, m_new, v_new, stat)
        w1_new = w1_new.reshape(2, d_model // 8, d_ff // 128, 8, 128).transpose(0, 1, 3, 2, 4).reshape(1, 2, 1, d_model, d_ff)
        w2_new = w2_new.reshape(2, d_ff // 8, d_model // 128, 8, 128).transpose(0, 1, 3, 2, 4).reshape(1, 2, 1, d_ff, d_model)
        flat_dims = (1, 2, 1, -1)
        return w1_new, w2_new, w_new.reshape(flat_dims), m_new.reshape(flat_dims), v_new.reshape(flat_dims), loss.reshape(()) / n_tokens

    act_spec = P(None, "data", None)
    flat_spec = P("stage", None, None, "data")
    return jax.shard_map(device_step, mesh=mesh, in_specs=(act_spec, act_spec, P("stage"), P("stage"), flat_spec, flat_spec, flat_spec), out_specs=(P("stage"), P("stage"), flat_spec, flat_spec, flat_spec, P()), check_vma=False)
```

```python
import functools
import math
import jax
import jax.numpy as jnp
from jax import lax
from jax.experimental import pallas as pl
from jax.experimental.pallas import tpu as pltpu
from jax.sharding import PartitionSpec as P

BETA_ONE = 0.9
BETA_TWO = 0.999
ADAM_EPS = 1e-8
WEIGHT_DECAY = 0.1
ADAM_STEP = 1000


TILE = (8, 128)
TILES = 72
VMEM_LIMIT = 60 * 1024 * 1024
PART = 24
ORDERS = ((2, 1, 0), (1, 0, 2), (0, 2, 1))
HALF_PART = PART // 2
STREAMS = tuple((h, k, d) for h in (1, 0) for k in range(3) for d in range(2))
EARLY = len(STREAMS) // 2
MESH_ID = pl.DeviceIdType.MESH


def torus():
    stage = lax.axis_index("stage")
    me = lax.axis_index("data")
    coords = (me // 16, (me // 4) % 4, me % 4)
    strides = (16, 4, 1)

    def ring(axis, delta):
        return lax.rem(coords[axis] + delta + 8, 4)

    def peer(axis, delta):
        return (stage, me + (ring(axis, delta) - coords[axis]) * strides[axis])

    return stage, me, coords, ring, peer


def sgn(d):
    return 1 - 2 * d


def pick(k, on_a, on_b, on_c):
    index = [on_a] * 3
    index[ORDERS[k][1]], index[ORDERS[k][2]] = on_b, on_c
    return tuple(index)


def remote(src, dst, send_sem, recv_sem, target):
    return pltpu.make_async_remote_copy(src_ref=src, dst_ref=dst, send_sem=send_sem, recv_sem=recv_sem, device_id=target, device_id_type=MESH_ID)


def grad_view(g_ref, stream, ring, turns, i):
    h, k, d = stream
    on_a, on_b = ring(ORDERS[k][0], -sgn(d) * turns), ring(ORDERS[k][1], -sgn(d) * (1 + i))
    return g_ref.at[(h,) + pick(k, on_a, on_b, slice(None)) + (pl.ds(PART * k + HALF_PART * d, HALF_PART),)]


def tail_kernel(tau_clip, learn_rate, g_ref, early_ref, w_ref, m_ref, v_ref, loss_ref,
                w_out, m_out, v_out, stat_out, full_out,
                recv1, recv2, recv3, local, nbuf,
                s1, r1, s2, r2, s3, r3, l_sem, e_sem, ns, nr, in_sem,
                t1, q1, t2, q2, t3, q3):
    stage, me, coords, ring, peer = torus()
    streams = [(k, d) for k in range(3) for d in range(2)]

    def friend(phase, delta):
        far, near = divmod(delta, 4)
        if phase == 0:
            return (lax.rem(stage + far, 2), peer(2, near)[1])
        return (stage, peer(0, far)[1] + peer(1, near)[1] - me)

    sizes = (8, 16)
    barrier = pltpu.get_barrier_semaphore()
    for phase, size in enumerate(sizes):
        for delta in range(1, size):
            pl.semaphore_signal(barrier, inc=1, device_id=friend(phase, delta), device_id_type=MESH_ID)
    pl.semaphore_wait(barrier, sum(sizes) - len(sizes))

    def next_of(st, phase):
        h, k, d = STREAMS[st]
        return peer(ORDERS[k][phase], sgn(d))

    def back_of(st, phase, turns):
        h, k, d = STREAMS[st]
        return ring(ORDERS[k][phase], -sgn(d) * turns)

    def first_send(st, i):
        return remote(grad_view(g_ref, STREAMS[st], ring, 1, i), recv1.at[st, 0, i], s1.at[st, 0, i], r1.at[st, 0, i], next_of(st, 0))

    def first_load(st, i):
        return pltpu.make_async_copy(early_ref.at[st, i], recv1.at[st, 0, i], e_sem.at[st, i])

    def forward1(st, step, i):
        return remote(recv1.at[st, step, i], recv1.at[st, step + 1, i], s1.at[st, step + 1, i], r1.at[st, step + 1, i], next_of(st, 0))

    def arrived1(st, step, i):
        return remote(recv1.at[st, step, i], recv1.at[st, step, i], s1.at[st, step, i], r1.at[st, step, i], next_of(st, 0))

    def fetch(st, n):
        return pltpu.make_async_copy(grad_view(g_ref, STREAMS[st], ring, 2 + n // 4, n % 4), local.at[st, n % 2], l_sem.at[st, n % 2])

    def send2(st, step):
        src = recv1.at[st, 2, 0] if step == 0 else recv2.at[st, step - 1]
        return remote(src, recv2.at[st, step], s2.at[st, step], r2.at[st, step], next_of(st, 1))

    def send3(st, step):
        src = recv2.at[st, 2, back_of(st, 2, 1)] if step == 0 else recv3.at[st, step - 1]
        return remote(src, recv3.at[st, step], s3.at[st, step], r3.at[st, step], next_of(st, 2))

    state_in = [pltpu.make_async_copy(src, dst, in_sem.at[j]) for j, (src, dst) in enumerate(((w_ref, w_out), (m_ref, m_out), (v_ref, v_out)))]
    all_st = range(len(STREAMS))
    early, late = all_st[:EARLY], all_st[EARLY:]
    for i in range(4):
        for st in early:
            first_load(st, i).start()
        for st in late:
            first_send(st, i).start()
        if i == 0:
            for st in all_st:
                for n in range(2):
                    fetch(st, n).start()

    for copy in state_in:
        copy.start()

    def accumulate(st, step, i, more):
        n = step * 4 + i
        if step == 0 and st < EARLY:
            first_load(st, i).wait()
        else:
            arrived1(st, step, i).wait_recv()
        fetch(st, n).wait()
        recv1[st, step, i] = recv1[st, step, i] + local[st, n % 2]
        if more:
            fetch(st, n + 2).start()

    for step in range(2):
        def phase1(i, carry):
            for st in all_st:
                accumulate(st, step, i, True)
                forward1(st, step, i).start()
            return carry

        lax.fori_loop(0, 4, phase1, 0)
    for i in range(4):
        for st in all_st:
            accumulate(st, 2, i, i < 2)
            if i == 0:
                send2(st, 0).start()
        if i > 0:
            for st in all_st:
                send2(st, i - 1).wait_recv()
                recv2[st, i - 1] = recv2[st, i - 1] + recv1[st, 2, i]
                if i < 3:
                    send2(st, i).start()
                else:
                    send3(st, 0).start()
    for step in range(3):
        for st in all_st:
            send3(st, step).wait_recv()
            recv3[st, step] = recv3[st, step] + recv2[st, 2, back_of(st, 2, 2 + step)]
            if step < 2:
                send3(st, step + 1).start()

    for copy in state_in:
        copy.wait()
    total = jnp.zeros(TILE, jnp.float32)
    for st in all_st:
        piece = recv3[st, 2]
        total = total + jnp.sum(piece * piece, axis=0)

    parts = (total, loss_ref[...])
    for phase, size in enumerate(sizes):
        mine = (stage * 4 + coords[2], coords[0] * 4 + coords[1])[phase]
        nbuf[phase, mine, 0], nbuf[phase, mine, 1] = parts
        sends = [remote(nbuf.at[phase, mine], nbuf.at[phase, mine], ns.at[phase, delta], nr.at[phase, delta], friend(phase, delta)) for delta in range(1, size)]
        for send in sends:
            send.start()
        for send in sends:
            send.wait_recv()
        parts = tuple(sum((nbuf[phase, slot, j] for slot in range(1, size)), nbuf[phase, 0, j]) for j in range(2))
        for send in sends:
            send.wait_send()

    stat_out[0] = jnp.sum(parts[1])
    norm = jnp.sqrt(jnp.full((8, 128), jnp.sum(parts[0]), jnp.float32))
    clip = jnp.minimum(1.0, tau_clip / norm)

    def update(width):
        def group(k, carry):
            for h in range(2):
                for t in range(PART):
                    rows = pl.ds(k * 192 + (t // width) * (8 * width) + t % width, 8, stride=width)
                    grad = clip * recv3[(1 - h) * EARLY + 2 * k + t // HALF_PART, 2, t % HALF_PART]
                    m_new = BETA_ONE * m_out[h, rows, :] + (1.0 - BETA_ONE) * grad
                    v_new = BETA_TWO * v_out[h, rows, :] + (1.0 - BETA_TWO) * grad * grad
                    m_hat = m_new * (1.0 / (1.0 - BETA_ONE ** ADAM_STEP))
                    v_hat = v_new * (1.0 / (1.0 - BETA_TWO ** ADAM_STEP))
                    w_old = w_out[h, rows, :]
                    w_new = w_old - learn_rate * (m_hat / (jnp.sqrt(v_hat) + ADAM_EPS) + WEIGHT_DECAY * w_old)
                    w_out[h, rows, :] = w_new
                    m_out[h, rows, :] = m_new
                    v_out[h, rows, :] = v_new
                    full_out[(h,) + coords + (k * PART + t,)] = w_new.astype(jnp.bfloat16)
            return carry

        lax.fori_loop(0, 3, group, 0)

    @pl.when(me < 32)
    def _():
        update(24)

    @pl.when(me >= 32)
    def _():
        update(6)

    def full_part(st, on_a, on_b, on_c):
        k, d = streams[st]
        return full_out.at[(d,) + pick(k, on_a, on_b, on_c) + (pl.ds(PART * k, PART),)]

    def along(st, phase):
        k, d = streams[st]
        return peer(ORDERS[k][phase], sgn(d))

    def coord_of(st, phase, delta):
        k, d = streams[st]
        return ring(ORDERS[k][phase], -sgn(d) * delta)

    def gather1(st, step):
        k, d = streams[st]
        place = full_part(st, coord_of(st, 0, 0), coord_of(st, 1, 0), coord_of(st, 2, step))
        return remote(place, place, t1.at[st, step], q1.at[st, step], along(st, 2))

    def gather2(st, step):
        place = full_part(st, coord_of(st, 0, 0), coord_of(st, 1, step), slice(None))
        return remote(place, place, t2.at[st, step], q2.at[st, step], along(st, 1))

    def gather3(st, step, i):
        place = full_part(st, coord_of(st, 0, step), coord_of(st, 1, i), slice(None))
        return remote(place, place, t3.at[st, step, i], q3.at[st, step, i], along(st, 0))

    for st in range(6):
        gather1(st, 0).start()
    for step in range(3):
        for st in range(6):
            gather1(st, step).wait_recv()
            if step < 2:
                gather1(st, step + 1).start()
    for st in range(6):
        gather2(st, 0).start()
        gather3(st, 0, 0).start()
    for step in range(3):
        for st in range(6):
            gather2(st, step).wait_recv()
            if step < 2:
                gather2(st, step + 1).start()
            gather3(st, 0, step + 1).start()

    def phase3(n, carry):
        step, i = n // 4, n % 4
        for st in range(6):
            gather3(st, step, i).wait_recv()
            gather3(st, step + 1, i).start()
        return carry

    lax.fori_loop(0, 8, phase3, 0)
    for i in range(4):
        for st in range(6):
            gather3(st, 2, i).wait_recv()

    def drain(i, carry):
        for step in range(3):
            for st in all_st:
                if step > 0 or st >= EARLY:
                    arrived1(st, step, i).wait_send()
            for st in range(6):
                gather3(st, step, i).wait_send()
        return carry

    lax.fori_loop(0, 4, drain, 0)
    for step in range(3):
        for st in all_st:
            send2(st, step).wait_send()
            send3(st, step).wait_send()
        for st in range(6):
            gather1(st, step).wait_send()
            gather2(st, step).wait_send()


def tail(grads, early, w_flat, m_flat, v_flat, loss_tile, tau_clip, learn_rate):
    f32, bf16 = jnp.float32, jnp.bfloat16
    flat = pltpu.VMEM(w_flat.shape, f32)
    in_vmem = pl.BlockSpec(memory_space=pltpu.VMEM)
    in_any = pl.BlockSpec(memory_space=pl.ANY)
    dma = pltpu.SemaphoreType.DMA
    n_stream = len(STREAMS)
    per_step = (n_stream, 3)
    per_sub = per_step + (4,)
    part = (HALF_PART,) + TILE
    per_place = (6, 3)
    return pl.pallas_call(
        functools.partial(tail_kernel, tau_clip, learn_rate),
        out_shape=(flat, flat, flat, jax.ShapeDtypeStruct((1,), f32), pltpu.VMEM(grads.shape, bf16)),
        in_specs=[in_any] * 5 + [in_vmem],
        out_specs=(in_vmem, in_vmem, in_vmem, pl.BlockSpec(memory_space=pltpu.SMEM), in_vmem),
        scratch_shapes=[
            pltpu.VMEM(per_sub + (4,) + part, f32),
            pltpu.VMEM(per_sub + part, f32),
            pltpu.VMEM(per_step + part, f32),
            pltpu.VMEM((n_stream, 2, 4) + part, f32),
            pltpu.VMEM((2, 16, 2) + TILE, f32),
            *[dma(per_sub)] * 2, *[dma(per_step)] * 4,
            dma((n_stream, 2)), dma((EARLY, 4)), *[dma((2, 16))] * 2, dma((3,)),
            *[dma(per_place)] * 4, *[dma(per_place + (4,))] * 2,
        ],
        compiler_params=pltpu.CompilerParams(collective_id=1, has_side_effects=True, vmem_limit_bytes=VMEM_LIMIT * 7 // 10),
        name="tail",
    )(grads, early, w_flat, m_flat, v_flat, loss_tile)


ROWS = 256
SLOTS = 4
BAND = 256
GELU_K = math.sqrt(2.0 / math.pi)
GELU_C = 0.044715


def gelu_tanh(pre, square):
    return jnp.tanh(pre * (GELU_K + (GELU_K * GELU_C) * square))


def stack_kernel(n_tokens, x_hbm, t_hbm, w1_hbm, w2_hbm, g_out, early_out, loss_out,
                 w1, w2, xs, gs, us, acts, rs, outf, outb, tgt, xt, stage1, stage2,
                 w1_sem, w2_sem, x_sem, t_sem, xsend, xrecv, gsend, grecv, o1_sem, o2_sem, es, er):
    stage, me, coords, ring, peer = torus()
    partner = (1 - stage, me)
    n_half, d_model, d_ff = w1.shape

    def load_w1(h):
        return pltpu.make_async_copy(w1_hbm.at[h], w1.at[h], w1_sem.at[h])

    def load_w2(h):
        return pltpu.make_async_copy(w2_hbm.at[h], w2.at[h], w2_sem.at[h])

    load_x = pltpu.make_async_copy(x_hbm, xs.at[0], x_sem)
    load_t = pltpu.make_async_copy(t_hbm, tgt, t_sem)

    @pl.when(stage == 0)
    def _():
        load_x.start()

    load_w1(0).start()

    barrier = pltpu.get_barrier_semaphore()
    pl.semaphore_signal(barrier, inc=1, device_id=partner, device_id_type=MESH_ID)
    for axis in range(3):
        for d in range(2):
            pl.semaphore_signal(barrier, inc=1, device_id=peer(axis, sgn(d)), device_id_type=MESH_ID)
    pl.semaphore_wait(barrier, 7)

    load_w2(0).start()

    @pl.when(stage == 0)
    def _():
        load_x.wait()

    loss_out[...] = jnp.zeros((8, 128), jnp.float32)

    def dot(lhs, rhs, on_left, on_right):
        return lax.dot_general(lhs, rhs, (((on_left,), (on_right,)), ((), ())), preferred_element_type=jnp.float32)

    def rows_of(c):
        return pl.ds(pl.multiple_of(c * ROWS, ROWS), ROWS)

    def block(i, size):
        return pl.ds(pl.multiple_of(i * size, size), size)

    def send_x(h, c, n):
        cols = block(n, BAND)
        return remote(outf.at[h, c, :, cols], xs.at[h + stage, rows_of(c), cols], xsend.at[h, c, n], xrecv.at[h + stage, c, n], partner)

    def wait_x(h, c, n):
        cols = block(n, BAND)
        remote(outf.at[h, c, :, cols], xs.at[h, rows_of(c), cols], xsend.at[h, c, n], xrecv.at[h, c, n], partner).wait_recv()

    def send_g(h, c, n):
        to, cols = h - 1 + stage, block(n, BAND)
        return remote(outb.at[h, c, :, cols], gs.at[to, rows_of(c), cols], gsend.at[h, c, n], grecv.at[to, c, n], partner)

    def wait_g(h, c, n):
        cols = block(n, BAND)
        remote(outb.at[h, c, :, cols], gs.at[h, rows_of(c), cols], gsend.at[h, c, n], grecv.at[h, c, n], partner).wait_recv()

    def forward(item, carry):
        h, c = item // 2, item % 2
        rows = rows_of(c)

        @pl.when(c == 0)
        def _():
            load_w1(h).wait()

        @pl.when(h + stage > 0)
        def _():
            for n in range(3):
                wait_x(h, c, n)

        def up(f, inner):
            cols = block(f, 512)
            pre = dot(xs[h, rows, :], w1[h, :, cols], 1, 0)
            us[h, rows, cols] = pre
            half = 0.5 * pre
            acts[h, rows, cols] = (half + half * gelu_tanh(pre, pre * pre)).astype(jnp.bfloat16)
            return inner

        lax.fori_loop(0, d_ff // 512, up, 0, unroll=True)

        @pl.when(c == 0)
        def _():
            load_w2(h).wait()

        @pl.when(item == 0)
        def _():
            load_w1(1).start()
            load_w2(1).start()
            load_t.start()

        def down(n, inner):
            cols = block(n, BAND)
            val = dot(acts[h, rows, :], w2[h, :, cols], 1, 0)
            outf[h, c, :, cols] = (xs[h, rows, cols].astype(jnp.float32) + val).astype(jnp.bfloat16)

            @pl.when(h + stage < 2)
            def _():
                send_x(h, c, n).start()

            return inner

        lax.fori_loop(0, d_model // BAND, down, 0)

        @pl.when(h + stage == 2)
        def _():
            @pl.when(c == 0)
            def _():
                load_t.wait()

            residual = outf[h, c].astype(jnp.float32) - tgt[rows, :].astype(jnp.float32)
            gs[h, rows, :] = (residual / n_tokens).astype(jnp.bfloat16)
            square = residual * residual
            part = sum(square[:, 128 * j:128 * (j + 1)] for j in range(d_model // 128))
            loss_out[...] += 0.5 * jnp.sum(part.reshape(ROWS // 8, 8, 128), axis=0)

        return carry

    lax.fori_loop(0, 2 * n_half, forward, 0)

    @pl.when(stage == 0)
    def _():
        load_t.wait()

    def out_one(h, n, i):
        return pltpu.make_async_copy(stage1.at[n % SLOTS, i], g_out.at[h, pl.ds(0, 2), :, :, pl.ds(i * 24 + 2 * n, 2)], o1_sem.at[n % SLOTS, i])

    def out_two(h, m):
        return pltpu.make_async_copy(stage2.at[m % SLOTS], g_out.at[h, 2 + m // 4, m % 4], o2_sem.at[m % SLOTS])

    def early_send(st, i):
        h, k, d = STREAMS[st]
        return remote(grad_view(g_out, STREAMS[st], ring, 1, i), early_out.at[st, i], es.at[st, i], er.at[st, i], peer(ORDERS[k][0], sgn(d)))

    def backward(b, carry):
        h = 1 - b

        def chain(c, inner):
            rows = rows_of(c)

            @pl.when(h + stage < 2)
            def _():
                for n in range(3):
                    wait_g(h, c, n)

            def up(f, deep):
                cols = block(f, 512)
                q = dot(gs[h, rows, :], w2[h, cols, :], 1, 1)
                pre = us[h, rows, cols]
                square = pre * pre
                th = gelu_tanh(pre, square)
                slope = (0.5 + 0.5 * th) + (1.0 - th * th) * (pre * (0.5 * GELU_K + (1.5 * GELU_K * GELU_C) * square))
                rs[rows, cols] = (q * slope).astype(jnp.bfloat16)
                return deep

            lax.fori_loop(0, d_ff // 512, up, 0, unroll=True)

            @pl.when(h + stage > 0)
            def _():
                def down(n, deep):
                    cols = block(n, BAND)
                    val = dot(rs[rows, :], w1[h, cols, :], 1, 1)
                    outb[h, c, :, cols] = (gs[h, rows, cols].astype(jnp.float32) + val).astype(jnp.bfloat16)
                    send_g(h, c, n).start()
                    return deep

                lax.fori_loop(0, d_model // BAND, down, 0)

            return inner

        lax.fori_loop(0, 2, chain, 0)

        xt[...] = xs[h].T

        def grad_one(n, inner):
            @pl.when(n >= SLOTS)
            def _():
                for i in range(3):
                    out_one(h, n, i).wait()

            val = dot(xt[...], rs[:, block(n, BAND)], 1, 0)
            for p in range(32):
                for i in range(3):
                    for j in range(2):
                        stage1[n % SLOTS, i, p // 16, (p // 4) % 4, p % 4, j] = val[p * 24 + i * 8:p * 24 + i * 8 + 8, 128 * j:128 * (j + 1)]
            for i in range(3):
                out_one(h, n, i).start()
            return inner

        lax.fori_loop(0, d_ff // BAND, grad_one, 0)

        def grad_two(m, inner):
            @pl.when(m >= SLOTS)
            def _():
                out_two(h, m).wait()

            val = dot(acts[h, :, block(m, 384)], gs[h], 0, 0)
            for p in range(4):
                for i in range(12):
                    for j in range(6):
                        stage2[m % SLOTS, p, i * 6 + j] = val[p * 96 + i * 8:p * 96 + i * 8 + 8, 128 * j:128 * (j + 1)]
            out_two(h, m).start()
            return inner

        lax.fori_loop(0, d_ff // 384, grad_two, 0)
        for n in range(SLOTS):
            for i in range(3):
                out_one(h, n, i).wait()
            out_two(h, n).wait()

        @pl.when(b == 0)
        def _():
            for i in range(4):
                for st in range(EARLY):
                    early_send(st, i).start()

        return carry

    lax.fori_loop(0, n_half, backward, 0)
    for i in range(4):
        for st in range(EARLY):
            early_send(st, i).wait()

    for h in range(2):
        for c in range(2):
            @pl.when(h + stage < 2)
            def _():
                for n in range(3):
                    send_x(h, c, n).wait_send()

            @pl.when(h + stage > 0)
            def _():
                for n in range(3):
                    send_g(h, c, n).wait_send()


def stack(x_all, t_all, w1, w2, n_tokens):
    rows, d_model = x_all.shape
    d_ff = w1.shape[2]
    bf16, f32 = jnp.bfloat16, jnp.float32
    dma = pltpu.SemaphoreType.DMA
    in_any = pl.BlockSpec(memory_space=pl.ANY)
    return pl.pallas_call(
        functools.partial(stack_kernel, n_tokens),
        out_shape=(jax.ShapeDtypeStruct((2, 4, 4, 4, TILES) + TILE, f32), jax.ShapeDtypeStruct((EARLY, 4, 4, HALF_PART) + TILE, f32), jax.ShapeDtypeStruct(TILE, f32)),
        in_specs=[in_any] * 4,
        out_specs=(in_any, in_any, pl.BlockSpec(memory_space=pltpu.VMEM)),
        scratch_shapes=[
            pltpu.VMEM((2, d_model, d_ff), bf16), pltpu.VMEM((2, d_ff, d_model), bf16),
            pltpu.VMEM((2, rows, d_model), bf16), pltpu.VMEM((2, rows, d_model), bf16),
            pltpu.VMEM((2, rows, d_ff), f32), pltpu.VMEM((2, rows, d_ff), bf16), pltpu.VMEM((rows, d_ff), bf16),
            pltpu.VMEM((2, 2, ROWS, d_model), bf16), pltpu.VMEM((2, 2, ROWS, d_model), bf16), pltpu.VMEM((rows, d_model), bf16), pltpu.VMEM((d_model, rows), bf16),
            pltpu.VMEM((SLOTS, 3, 2, 4, 4, 2) + TILE, f32), pltpu.VMEM((SLOTS, 4, TILES) + TILE, f32),
            dma((2,)), dma((2,)), dma, dma, *[dma((2, 2, 3))] * 4, dma((SLOTS, 3)), dma((SLOTS,)), *[dma((EARLY, 4))] * 2,
        ],
        compiler_params=pltpu.CompilerParams(collective_id=0, has_side_effects=True, vmem_limit_bytes=VMEM_LIMIT),
        name="stack",
    )(x_all, t_all, w1, w2)


def solution(mesh):
    n_stage = mesh.shape["stage"]
    n_data = mesh.shape["data"]

    def device_step(x_loc, t_loc, w1_loc, w2_loc, wm_loc, m_loc, v_loc):
        n_micro, n_tok, d_model = x_loc.shape
        d_ff = w1_loc.shape[4]
        n_tokens = n_micro * n_tok * n_data
        n_blocks = 2 * n_stage
        tau_clip = 0.3 * d_model * math.sqrt(n_blocks * (3.0 / n_tokens + 0.008))
        learn_rate = 0.1 / math.sqrt(4.0 * d_model * n_blocks)
        x_all = x_loc.reshape(n_micro * n_tok, d_model)
        t_all = t_loc.reshape(n_micro * n_tok, d_model)
        grads, early, loss_tile = stack(x_all, t_all, w1_loc[0, :, 0], w2_loc[0, :, 0], n_tokens)
        w_new, m_new, v_new, stat, w_full = tail(
            grads, early, wm_loc.reshape(2, 576, 128), m_loc.reshape(2, 576, 128), v_loc.reshape(2, 576, 128),
            loss_tile, tau_clip, learn_rate)
        w1_new = w_full[:, :2].reshape(2, d_model // 8, d_ff // 128, 8, 128).transpose(0, 1, 3, 2, 4).reshape(1, 2, 1, d_model, d_ff)
        w2_new = w_full[:, 2:].reshape(2, d_ff // 8, d_model // 128, 8, 128).transpose(0, 1, 3, 2, 4).reshape(1, 2, 1, d_ff, d_model)
        flat_dims = (1, 2, 1, -1)
        return w1_new, w2_new, w_new.reshape(flat_dims), m_new.reshape(flat_dims), v_new.reshape(flat_dims), stat.reshape(()) / n_tokens

    act_spec = P(None, "data", None)
    flat_spec = P("stage", None, None, "data")
    return jax.shard_map(device_step, mesh=mesh, in_specs=(act_spec, act_spec, P("stage"), P("stage"), flat_spec, flat_spec, flat_spec), out_specs=(P("stage"), P("stage"), flat_spec, flat_spec, flat_spec, P()), check_vma=False)
```

```python
import functools
import math
import jax
import jax.numpy as jnp
from jax import lax
from jax.experimental import pallas as pl
from jax.experimental.pallas import tpu as pltpu
from jax.sharding import PartitionSpec as P

BETA_ONE = 0.9
BETA_TWO = 0.999
ADAM_EPS = 1e-8
WEIGHT_DECAY = 0.1
ADAM_STEP = 1000


TILE = (8, 128)
TILES = 72
VMEM_LIMIT = 60 * 1024 * 1024
PART = 24
ORDERS = ((2, 1, 0), (1, 0, 2), (0, 2, 1))
HALF_PART = PART // 2
STREAMS = tuple((h, k, d) for h in (1, 0) for k in range(3) for d in range(2))
EARLY = len(STREAMS) // 2
MESH_ID = pl.DeviceIdType.MESH


def torus():
    stage = lax.axis_index("stage")
    me = lax.axis_index("data")
    coords = (me // 16, (me // 4) % 4, me % 4)
    strides = (16, 4, 1)

    def ring(axis, delta):
        return lax.rem(coords[axis] + delta + 8, 4)

    def peer(axis, delta):
        return (stage, me + (ring(axis, delta) - coords[axis]) * strides[axis])

    return stage, me, coords, ring, peer


def sgn(d):
    return 1 - 2 * d


def pick(k, on_a, on_b, on_c):
    index = [on_a] * 3
    index[ORDERS[k][1]], index[ORDERS[k][2]] = on_b, on_c
    return tuple(index)


def remote(src, dst, send_sem, recv_sem, target):
    return pltpu.make_async_remote_copy(src_ref=src, dst_ref=dst, send_sem=send_sem, recv_sem=recv_sem, device_id=target, device_id_type=MESH_ID)


def grad_view(g_ref, stream, ring, turns, i):
    h, k, d = stream
    on_a, on_b = ring(ORDERS[k][0], -sgn(d) * turns), ring(ORDERS[k][1], -sgn(d) * (1 + i))
    return g_ref.at[(h,) + pick(k, on_a, on_b, slice(None)) + (pl.ds(PART * k + HALF_PART * d, HALF_PART),)]


def tail_kernel(tau_clip, learn_rate, g_ref, early_ref, w_ref, m_ref, v_ref, loss_ref,
                w_out, m_out, v_out, stat_out, full_out,
                recv1, recv2, recv3, local, nbuf,
                s1, r1, s2, r2, s3, r3, l_sem, e_sem, ns, nr, in_sem,
                t1, q1, t2, q2, t3, q3):
    stage, me, coords, ring, peer = torus()
    streams = [(k, d) for k in range(3) for d in range(2)]

    def friend(phase, delta):
        far, near = divmod(delta, 4)
        if phase == 0:
            return (lax.rem(stage + far, 2), peer(2, near)[1])
        return (stage, peer(0, far)[1] + peer(1, near)[1] - me)

    sizes = (8, 16)
    barrier = pltpu.get_barrier_semaphore()
    for phase, size in enumerate(sizes):
        for delta in range(1, size):
            pl.semaphore_signal(barrier, inc=1, device_id=friend(phase, delta), device_id_type=MESH_ID)
    pl.semaphore_wait(barrier, sum(sizes) - len(sizes))

    def next_of(st, phase):
        h, k, d = STREAMS[st]
        return peer(ORDERS[k][phase], sgn(d))

    def back_of(st, phase, turns):
        h, k, d = STREAMS[st]
        return ring(ORDERS[k][phase], -sgn(d) * turns)

    def first_send(st, i):
        return remote(grad_view(g_ref, STREAMS[st], ring, 1, i), recv1.at[st, 0, i], s1.at[st, 0, i], r1.at[st, 0, i], next_of(st, 0))

    def first_load(st, i):
        return pltpu.make_async_copy(early_ref.at[st, i], recv1.at[st, 0, i], e_sem.at[st, i])

    def forward1(st, step, i):
        return remote(recv1.at[st, step, i], recv1.at[st, step + 1, i], s1.at[st, step + 1, i], r1.at[st, step + 1, i], next_of(st, 0))

    def arrived1(st, step, i):
        return remote(recv1.at[st, step, i], recv1.at[st, step, i], s1.at[st, step, i], r1.at[st, step, i], next_of(st, 0))

    def fetch(st, n):
        return pltpu.make_async_copy(grad_view(g_ref, STREAMS[st], ring, 2 + n // 4, n % 4), local.at[st, n % 2], l_sem.at[st, n % 2])

    def send2(st, step):
        src = recv1.at[st, 2, 0] if step == 0 else recv2.at[st, step - 1]
        return remote(src, recv2.at[st, step], s2.at[st, step], r2.at[st, step], next_of(st, 1))

    def send3(st, step):
        src = recv2.at[st, 2, back_of(st, 2, 1)] if step == 0 else recv3.at[st, step - 1]
        return remote(src, recv3.at[st, step], s3.at[st, step], r3.at[st, step], next_of(st, 2))

    state_in = [pltpu.make_async_copy(src, dst, in_sem.at[j]) for j, (src, dst) in enumerate(((w_ref, w_out), (m_ref, m_out), (v_ref, v_out)))]
    all_st = range(len(STREAMS))
    early, late = all_st[:EARLY], all_st[EARLY:]
    for st in early:
        first_load(st, 0).start()
    for i in range(2):
        for st in late:
            first_send(st, i).start()
    for st in all_st:
        for n in range(2):
            fetch(st, n).start()
    for i in range(1, 4):
        for st in early:
            first_load(st, i).start()
    for copy in state_in:
        copy.start()

    def accumulate(st, step, i, more):
        n = step * 4 + i
        if step == 0 and st < EARLY:
            first_load(st, i).wait()
        else:
            arrived1(st, step, i).wait_recv()
        fetch(st, n).wait()
        recv1[st, step, i] = recv1[st, step, i] + local[st, n % 2]
        if more:
            fetch(st, n + 2).start()

    def pass_on(group, step, i):
        for st in group:
            accumulate(st, step, i, True)
            forward1(st, step, i).start()

    def last_step(group, i):
        for st in group:
            accumulate(st, 2, i, i < 2)
            if i == 0:
                send2(st, 0).start()
        if i > 0:
            for st in group:
                send2(st, i - 1).wait_recv()
                recv2[st, i - 1] = recv2[st, i - 1] + recv1[st, 2, i]
                if i < 3:
                    send2(st, i).start()
                else:
                    send3(st, 0).start()

    def last_ring(group, step):
        for st in group:
            send3(st, step).wait_recv()
            recv3[st, step] = recv3[st, step] + recv2[st, 2, back_of(st, 2, 2 + step)]
            if step < 2:
                send3(st, step + 1).start()

    def lead(i, carry):
        pass_on(early, 0, i)
        return carry

    def both(i, carry):
        pass_on(early, 1, i)
        pass_on(late, 0, i)
        return carry

    lax.fori_loop(0, 4, lead, 0)
    for i in range(2, 4):
        for st in late:
            first_send(st, i).start()
    lax.fori_loop(0, 4, both, 0)
    for i in range(4):
        last_step(early, i)
        pass_on(late, 1, i)
    for i in range(4):
        if i < 3:
            last_ring(early, i)
        last_step(late, i)
    for step in range(3):
        last_ring(late, step)

    for copy in state_in:
        copy.wait()
    total = jnp.zeros(TILE, jnp.float32)
    for st in all_st:
        piece = recv3[st, 2]
        total = total + jnp.sum(piece * piece, axis=0)

    parts = (total, loss_ref[...])
    for phase, size in enumerate(sizes):
        mine = (stage * 4 + coords[2], coords[0] * 4 + coords[1])[phase]
        nbuf[phase, mine, 0], nbuf[phase, mine, 1] = parts
        sends = [remote(nbuf.at[phase, mine], nbuf.at[phase, mine], ns.at[phase, delta], nr.at[phase, delta], friend(phase, delta)) for delta in range(1, size)]
        for send in sends:
            send.start()
        for send in sends:
            send.wait_recv()
        parts = tuple(sum((nbuf[phase, slot, j] for slot in range(1, size)), nbuf[phase, 0, j]) for j in range(2))
        for send in sends:
            send.wait_send()

    stat_out[0] = jnp.sum(parts[1])
    norm = jnp.sqrt(jnp.full((8, 128), jnp.sum(parts[0]), jnp.float32))
    clip = jnp.minimum(1.0, tau_clip / norm)

    def update(width):
        def group(k, carry):
            for h in range(2):
                for t in range(PART):
                    rows = pl.ds(k * 192 + (t // width) * (8 * width) + t % width, 8, stride=width)
                    grad = clip * recv3[(1 - h) * EARLY + 2 * k + t // HALF_PART, 2, t % HALF_PART]
                    m_new = BETA_ONE * m_out[h, rows, :] + (1.0 - BETA_ONE) * grad
                    v_new = BETA_TWO * v_out[h, rows, :] + (1.0 - BETA_TWO) * grad * grad
                    m_hat = m_new * (1.0 / (1.0 - BETA_ONE ** ADAM_STEP))
                    v_hat = v_new * (1.0 / (1.0 - BETA_TWO ** ADAM_STEP))
                    w_old = w_out[h, rows, :]
                    w_new = w_old - learn_rate * (m_hat / (jnp.sqrt(v_hat) + ADAM_EPS) + WEIGHT_DECAY * w_old)
                    w_out[h, rows, :] = w_new
                    m_out[h, rows, :] = m_new
                    v_out[h, rows, :] = v_new
                    full_out[(h,) + coords + (k * PART + t,)] = w_new.astype(jnp.bfloat16)
            return carry

        lax.fori_loop(0, 3, group, 0)

    @pl.when(me < 32)
    def _():
        update(24)

    @pl.when(me >= 32)
    def _():
        update(6)

    def full_part(st, on_a, on_b, on_c):
        k, d = streams[st]
        return full_out.at[(d,) + pick(k, on_a, on_b, on_c) + (pl.ds(PART * k, PART),)]

    def along(st, phase):
        k, d = streams[st]
        return peer(ORDERS[k][phase], sgn(d))

    def coord_of(st, phase, delta):
        k, d = streams[st]
        return ring(ORDERS[k][phase], -sgn(d) * delta)

    def gather1(st, step):
        k, d = streams[st]
        place = full_part(st, coord_of(st, 0, 0), coord_of(st, 1, 0), coord_of(st, 2, step))
        return remote(place, place, t1.at[st, step], q1.at[st, step], along(st, 2))

    def gather2(st, step):
        place = full_part(st, coord_of(st, 0, 0), coord_of(st, 1, step), slice(None))
        return remote(place, place, t2.at[st, step], q2.at[st, step], along(st, 1))

    def gather3(st, step, i):
        place = full_part(st, coord_of(st, 0, step), coord_of(st, 1, i), slice(None))
        return remote(place, place, t3.at[st, step, i], q3.at[st, step, i], along(st, 0))

    for st in range(6):
        gather1(st, 0).start()
    for step in range(3):
        for st in range(6):
            gather1(st, step).wait_recv()
            if step < 2:
                gather1(st, step + 1).start()
    for st in range(6):
        gather2(st, 0).start()
        gather3(st, 0, 0).start()
    for step in range(3):
        for st in range(6):
            gather2(st, step).wait_recv()
            if step < 2:
                gather2(st, step + 1).start()
            gather3(st, 0, step + 1).start()

    def phase3(n, carry):
        step, i = n // 4, n % 4
        for st in range(6):
            gather3(st, step, i).wait_recv()
            gather3(st, step + 1, i).start()
        return carry

    lax.fori_loop(0, 8, phase3, 0)
    for i in range(4):
        for st in range(6):
            gather3(st, 2, i).wait_recv()

    def drain(i, carry):
        for step in range(3):
            for st in all_st:
                if step > 0 or st >= EARLY:
                    arrived1(st, step, i).wait_send()
            for st in range(6):
                gather3(st, step, i).wait_send()
        return carry

    lax.fori_loop(0, 4, drain, 0)
    for step in range(3):
        for st in all_st:
            send2(st, step).wait_send()
            send3(st, step).wait_send()
        for st in range(6):
            gather1(st, step).wait_send()
            gather2(st, step).wait_send()


def tail(grads, early, w_flat, m_flat, v_flat, loss_tile, tau_clip, learn_rate):
    f32, bf16 = jnp.float32, jnp.bfloat16
    flat = pltpu.VMEM(w_flat.shape, f32)
    in_vmem = pl.BlockSpec(memory_space=pltpu.VMEM)
    in_any = pl.BlockSpec(memory_space=pl.ANY)
    dma = pltpu.SemaphoreType.DMA
    n_stream = len(STREAMS)
    per_step = (n_stream, 3)
    per_sub = per_step + (4,)
    part = (HALF_PART,) + TILE
    per_place = (6, 3)
    return pl.pallas_call(
        functools.partial(tail_kernel, tau_clip, learn_rate),
        out_shape=(flat, flat, flat, jax.ShapeDtypeStruct((1,), f32), pltpu.VMEM(grads.shape, bf16)),
        in_specs=[in_any] * 5 + [in_vmem],
        out_specs=(in_vmem, in_vmem, in_vmem, pl.BlockSpec(memory_space=pltpu.SMEM), in_vmem),
        scratch_shapes=[
            pltpu.VMEM(per_sub + (4,) + part, f32),
            pltpu.VMEM(per_sub + part, f32),
            pltpu.VMEM(per_step + part, f32),
            pltpu.VMEM((n_stream, 2, 4) + part, f32),
            pltpu.VMEM((2, 16, 2) + TILE, f32),
            *[dma(per_sub)] * 2, *[dma(per_step)] * 4,
            dma((n_stream, 2)), dma((EARLY, 4)), *[dma((2, 16))] * 2, dma((3,)),
            *[dma(per_place)] * 4, *[dma(per_place + (4,))] * 2,
        ],
        compiler_params=pltpu.CompilerParams(collective_id=1, has_side_effects=True, vmem_limit_bytes=VMEM_LIMIT * 7 // 10),
        name="tail",
    )(grads, early, w_flat, m_flat, v_flat, loss_tile)


ROWS = 256
SLOTS = 4
BAND = 256
GELU_K = math.sqrt(2.0 / math.pi)
GELU_C = 0.044715


def gelu_tanh(pre, square):
    return jnp.tanh(pre * (GELU_K + (GELU_K * GELU_C) * square))


def stack_kernel(n_tokens, x_hbm, t_hbm, w1_hbm, w2_hbm, g_out, early_out, loss_out,
                 w1, w2, xs, gs, us, acts, rs, outf, outb, tgt, xt, stage1, stage2,
                 w1_sem, w2_sem, x_sem, t_sem, xsend, xrecv, gsend, grecv, o1_sem, o2_sem, es, er):
    stage, me, coords, ring, peer = torus()
    partner = (1 - stage, me)
    n_half, d_model, d_ff = w1.shape

    def load_w1(h):
        return pltpu.make_async_copy(w1_hbm.at[h], w1.at[h], w1_sem.at[h])

    def load_w2(h):
        return pltpu.make_async_copy(w2_hbm.at[h], w2.at[h], w2_sem.at[h])

    load_x = pltpu.make_async_copy(x_hbm, xs.at[0], x_sem)
    load_t = pltpu.make_async_copy(t_hbm, tgt, t_sem)

    @pl.when(stage == 0)
    def _():
        load_x.start()

    load_w1(0).start()

    barrier = pltpu.get_barrier_semaphore()
    pl.semaphore_signal(barrier, inc=1, device_id=partner, device_id_type=MESH_ID)
    for axis in range(3):
        for d in range(2):
            pl.semaphore_signal(barrier, inc=1, device_id=peer(axis, sgn(d)), device_id_type=MESH_ID)
    pl.semaphore_wait(barrier, 7)

    load_w2(0).start()

    @pl.when(stage == 0)
    def _():
        load_x.wait()

    loss_out[...] = jnp.zeros((8, 128), jnp.float32)

    def dot(lhs, rhs, on_left, on_right):
        return lax.dot_general(lhs, rhs, (((on_left,), (on_right,)), ((), ())), preferred_element_type=jnp.float32)

    def rows_of(c):
        return pl.ds(pl.multiple_of(c * ROWS, ROWS), ROWS)

    def block(i, size):
        return pl.ds(pl.multiple_of(i * size, size), size)

    def send_x(h, c, n):
        cols = block(n, BAND)
        return remote(outf.at[h, c, :, cols], xs.at[h + stage, rows_of(c), cols], xsend.at[h, c, n], xrecv.at[h + stage, c, n], partner)

    def wait_x(h, c, n):
        cols = block(n, BAND)
        remote(outf.at[h, c, :, cols], xs.at[h, rows_of(c), cols], xsend.at[h, c, n], xrecv.at[h, c, n], partner).wait_recv()

    def send_g(h, c, n):
        to, cols = h - 1 + stage, block(n, BAND)
        return remote(outb.at[h, c, :, cols], gs.at[to, rows_of(c), cols], gsend.at[h, c, n], grecv.at[to, c, n], partner)

    def wait_g(h, c, n):
        cols = block(n, BAND)
        remote(outb.at[h, c, :, cols], gs.at[h, rows_of(c), cols], gsend.at[h, c, n], grecv.at[h, c, n], partner).wait_recv()

    def forward(item, carry):
        h, c = item // 2, item % 2
        rows = rows_of(c)

        @pl.when(c == 0)
        def _():
            load_w1(h).wait()

        @pl.when(h + stage > 0)
        def _():
            for n in range(3):
                wait_x(h, c, n)

        def up(f, inner):
            cols = block(f, 512)
            pre = dot(xs[h, rows, :], w1[h, :, cols], 1, 0)
            us[h, rows, cols] = pre
            half = 0.5 * pre
            acts[h, rows, cols] = (half + half * gelu_tanh(pre, pre * pre)).astype(jnp.bfloat16)
            return inner

        lax.fori_loop(0, d_ff // 512, up, 0, unroll=True)

        @pl.when(c == 0)
        def _():
            load_w2(h).wait()

        @pl.when(item == 0)
        def _():
            load_w1(1).start()
            load_w2(1).start()
            load_t.start()

        def down(n, inner):
            cols = block(n, BAND)
            val = dot(acts[h, rows, :], w2[h, :, cols], 1, 0)
            outf[h, c, :, cols] = (xs[h, rows, cols].astype(jnp.float32) + val).astype(jnp.bfloat16)

            @pl.when(h + stage < 2)
            def _():
                send_x(h, c, n).start()

            return inner

        lax.fori_loop(0, d_model // BAND, down, 0)

        @pl.when(h + stage == 2)
        def _():
            @pl.when(c == 0)
            def _():
                load_t.wait()

            residual = outf[h, c].astype(jnp.float32) - tgt[rows, :].astype(jnp.float32)
            gs[h, rows, :] = (residual / n_tokens).astype(jnp.bfloat16)
            square = residual * residual
            part = sum(square[:, 128 * j:128 * (j + 1)] for j in range(d_model // 128))
            loss_out[...] += 0.5 * jnp.sum(part.reshape(ROWS // 8, 8, 128), axis=0)

        return carry

    lax.fori_loop(0, 2 * n_half, forward, 0)

    @pl.when(stage == 0)
    def _():
        load_t.wait()

    def out_one(h, n, i):
        return pltpu.make_async_copy(stage1.at[n % SLOTS, i], g_out.at[h, pl.ds(0, 2), :, :, pl.ds(i * 24 + 2 * n, 2)], o1_sem.at[n % SLOTS, i])

    def out_two(h, m):
        return pltpu.make_async_copy(stage2.at[m % SLOTS], g_out.at[h, 2 + m // 4, m % 4], o2_sem.at[m % SLOTS])

    def early_send(st, i):
        h, k, d = STREAMS[st]
        return remote(grad_view(g_out, STREAMS[st], ring, 1, i), early_out.at[st, i], es.at[st, i], er.at[st, i], peer(ORDERS[k][0], sgn(d)))

    def backward(b, carry):
        h = 1 - b

        def chain(c, inner):
            rows = rows_of(c)

            @pl.when(h + stage < 2)
            def _():
                for n in range(3):
                    wait_g(h, c, n)

            def up(f, deep):
                cols = block(f, 512)
                q = dot(gs[h, rows, :], w2[h, cols, :], 1, 1)
                pre = us[h, rows, cols]
                square = pre * pre
                th = gelu_tanh(pre, square)
                slope = (0.5 + 0.5 * th) + (1.0 - th * th) * (pre * (0.5 * GELU_K + (1.5 * GELU_K * GELU_C) * square))
                rs[rows, cols] = (q * slope).astype(jnp.bfloat16)
                return deep

            lax.fori_loop(0, d_ff // 512, up, 0, unroll=True)

            @pl.when(h + stage > 0)
            def _():
                def down(n, deep):
                    cols = block(n, BAND)
                    val = dot(rs[rows, :], w1[h, cols, :], 1, 1)
                    outb[h, c, :, cols] = (gs[h, rows, cols].astype(jnp.float32) + val).astype(jnp.bfloat16)
                    send_g(h, c, n).start()
                    return deep

                lax.fori_loop(0, d_model // BAND, down, 0)

            return inner

        lax.fori_loop(0, 2, chain, 0)

        xt[...] = xs[h].T

        def grad_one(n, inner):
            @pl.when(n >= SLOTS)
            def _():
                for i in range(3):
                    out_one(h, n, i).wait()

            val = dot(xt[...], rs[:, block(n, BAND)], 1, 0)
            for p in range(32):
                for i in range(3):
                    for j in range(2):
                        stage1[n % SLOTS, i, p // 16, (p // 4) % 4, p % 4, j] = val[p * 24 + i * 8:p * 24 + i * 8 + 8, 128 * j:128 * (j + 1)]
            for i in range(3):
                out_one(h, n, i).start()
            return inner

        lax.fori_loop(0, d_ff // BAND, grad_one, 0)

        def grad_two(m, inner):
            @pl.when(m >= SLOTS)
            def _():
                out_two(h, m).wait()

            val = dot(acts[h, :, block(m, 384)], gs[h], 0, 0)
            for p in range(4):
                for i in range(12):
                    for j in range(6):
                        stage2[m % SLOTS, p, i * 6 + j] = val[p * 96 + i * 8:p * 96 + i * 8 + 8, 128 * j:128 * (j + 1)]
            out_two(h, m).start()
            return inner

        lax.fori_loop(0, d_ff // 384, grad_two, 0)
        for n in range(SLOTS):
            for i in range(3):
                out_one(h, n, i).wait()
            out_two(h, n).wait()

        @pl.when(b == 0)
        def _():
            for i in range(4):
                for st in range(EARLY):
                    early_send(st, i).start()

        return carry

    lax.fori_loop(0, n_half, backward, 0)
    for i in range(4):
        for st in range(EARLY):
            early_send(st, i).wait()

    for h in range(2):
        for c in range(2):
            @pl.when(h + stage < 2)
            def _():
                for n in range(3):
                    send_x(h, c, n).wait_send()

            @pl.when(h + stage > 0)
            def _():
                for n in range(3):
                    send_g(h, c, n).wait_send()


def stack(x_all, t_all, w1, w2, n_tokens):
    rows, d_model = x_all.shape
    d_ff = w1.shape[2]
    bf16, f32 = jnp.bfloat16, jnp.float32
    dma = pltpu.SemaphoreType.DMA
    in_any = pl.BlockSpec(memory_space=pl.ANY)
    return pl.pallas_call(
        functools.partial(stack_kernel, n_tokens),
        out_shape=(jax.ShapeDtypeStruct((2, 4, 4, 4, TILES) + TILE, f32), jax.ShapeDtypeStruct((EARLY, 4, 4, HALF_PART) + TILE, f32), jax.ShapeDtypeStruct(TILE, f32)),
        in_specs=[in_any] * 4,
        out_specs=(in_any, in_any, pl.BlockSpec(memory_space=pltpu.VMEM)),
        scratch_shapes=[
            pltpu.VMEM((2, d_model, d_ff), bf16), pltpu.VMEM((2, d_ff, d_model), bf16),
            pltpu.VMEM((2, rows, d_model), bf16), pltpu.VMEM((2, rows, d_model), bf16),
            pltpu.VMEM((2, rows, d_ff), f32), pltpu.VMEM((2, rows, d_ff), bf16), pltpu.VMEM((rows, d_ff), bf16),
            pltpu.VMEM((2, 2, ROWS, d_model), bf16), pltpu.VMEM((2, 2, ROWS, d_model), bf16), pltpu.VMEM((rows, d_model), bf16), pltpu.VMEM((d_model, rows), bf16),
            pltpu.VMEM((SLOTS, 3, 2, 4, 4, 2) + TILE, f32), pltpu.VMEM((SLOTS, 4, TILES) + TILE, f32),
            dma((2,)), dma((2,)), dma, dma, *[dma((2, 2, 3))] * 4, dma((SLOTS, 3)), dma((SLOTS,)), *[dma((EARLY, 4))] * 2,
        ],
        compiler_params=pltpu.CompilerParams(collective_id=0, has_side_effects=True, vmem_limit_bytes=VMEM_LIMIT),
        name="stack",
    )(x_all, t_all, w1, w2)


def solution(mesh):
    n_stage = mesh.shape["stage"]
    n_data = mesh.shape["data"]

    def device_step(x_loc, t_loc, w1_loc, w2_loc, wm_loc, m_loc, v_loc):
        n_micro, n_tok, d_model = x_loc.shape
        d_ff = w1_loc.shape[4]
        n_tokens = n_micro * n_tok * n_data
        n_blocks = 2 * n_stage
        tau_clip = 0.3 * d_model * math.sqrt(n_blocks * (3.0 / n_tokens + 0.008))
        learn_rate = 0.1 / math.sqrt(4.0 * d_model * n_blocks)
        x_all = x_loc.reshape(n_micro * n_tok, d_model)
        t_all = t_loc.reshape(n_micro * n_tok, d_model)
        grads, early, loss_tile = stack(x_all, t_all, w1_loc[0, :, 0], w2_loc[0, :, 0], n_tokens)
        w_new, m_new, v_new, stat, w_full = tail(
            grads, early, wm_loc.reshape(2, 576, 128), m_loc.reshape(2, 576, 128), v_loc.reshape(2, 576, 128),
            loss_tile, tau_clip, learn_rate)
        w1_new = w_full[:, :2].reshape(2, d_model // 8, d_ff // 128, 8, 128).transpose(0, 1, 3, 2, 4).reshape(1, 2, 1, d_model, d_ff)
        w2_new = w_full[:, 2:].reshape(2, d_ff // 8, d_model // 128, 8, 128).transpose(0, 1, 3, 2, 4).reshape(1, 2, 1, d_ff, d_model)
        flat_dims = (1, 2, 1, -1)
        return w1_new, w2_new, w_new.reshape(flat_dims), m_new.reshape(flat_dims), v_new.reshape(flat_dims), stat.reshape(()) / n_tokens

    act_spec = P(None, "data", None)
    flat_spec = P("stage", None, None, "data")
    return jax.shard_map(device_step, mesh=mesh, in_specs=(act_spec, act_spec, P("stage"), P("stage"), flat_spec, flat_spec, flat_spec), out_specs=(P("stage"), P("stage"), flat_spec, flat_spec, flat_spec, P()), check_vma=False)
```

```python
import functools
import math
import jax
import jax.numpy as jnp
from jax import lax
from jax.experimental import pallas as pl
from jax.experimental.pallas import tpu as pltpu
from jax.sharding import PartitionSpec as P

BETA_ONE = 0.9
BETA_TWO = 0.999
ADAM_EPS = 1e-8
WEIGHT_DECAY = 0.1
ADAM_STEP = 1000


TILE = (8, 128)
TILES = 72
VMEM_LIMIT = 60 * 1024 * 1024
PART = 24
ORDERS = ((2, 1, 0), (1, 0, 2), (0, 2, 1))
HALF_PART = PART // 2
STREAMS = tuple((h, k, d) for h in (1, 0) for k in range(3) for d in range(2))
EARLY = len(STREAMS) // 2
MESH_ID = pl.DeviceIdType.MESH


def torus():
    stage = lax.axis_index("stage")
    me = lax.axis_index("data")
    coords = (me // 16, (me // 4) % 4, me % 4)
    strides = (16, 4, 1)

    def ring(axis, delta):
        return lax.rem(coords[axis] + delta + 8, 4)

    def peer(axis, delta):
        return (stage, me + (ring(axis, delta) - coords[axis]) * strides[axis])

    return stage, me, coords, ring, peer


def sgn(d):
    return 1 - 2 * d


def pick(k, on_a, on_b, on_c):
    index = [on_a] * 3
    index[ORDERS[k][1]], index[ORDERS[k][2]] = on_b, on_c
    return tuple(index)


def remote(src, dst, send_sem, recv_sem, target):
    return pltpu.make_async_remote_copy(src_ref=src, dst_ref=dst, send_sem=send_sem, recv_sem=recv_sem, device_id=target, device_id_type=MESH_ID)


def grad_view(g_ref, stream, ring, turns, i):
    h, k, d = stream
    on_a, on_b = ring(ORDERS[k][0], -sgn(d) * turns), ring(ORDERS[k][1], -sgn(d) * (1 + i))
    return g_ref.at[(h,) + pick(k, on_a, on_b, slice(None)) + (pl.ds(PART * k + HALF_PART * d, HALF_PART),)]


def tail_kernel(tau_clip, learn_rate, g_ref, early_ref, w_ref, m_ref, v_ref, loss_ref,
                state, stat_out, full_out,
                recv1, recv2, recv3, local, nbuf,
                s1, r1, s2, r2, s3, r3, l_sem, e_sem, ns, nr, in_sem,
                t1, q1, t2, q2, t3, q3):
    stage, me, coords, ring, peer = torus()
    streams = [(k, d) for k in range(3) for d in range(2)]

    def friend(phase, delta):
        far, near = divmod(delta, 4)
        if phase == 0:
            return (lax.rem(stage + far, 2), peer(2, near)[1])
        return (stage, peer(0, far)[1] + peer(1, near)[1] - me)

    sizes = (8, 16)
    barrier = pltpu.get_barrier_semaphore()
    for phase, size in enumerate(sizes):
        for delta in range(1, size):
            pl.semaphore_signal(barrier, inc=1, device_id=friend(phase, delta), device_id_type=MESH_ID)

    def next_of(st, phase):
        h, k, d = STREAMS[st]
        return peer(ORDERS[k][phase], sgn(d))

    def back_of(st, phase, turns):
        h, k, d = STREAMS[st]
        return ring(ORDERS[k][phase], -sgn(d) * turns)

    def first_send(st, i):
        return remote(grad_view(g_ref, STREAMS[st], ring, 1, i), recv1.at[st, 0, i], s1.at[st, 0, i], r1.at[st, 0, i], next_of(st, 0))

    def first_load(st, i):
        return pltpu.make_async_copy(early_ref.at[st, i], recv1.at[st, 0, i], e_sem.at[st, i])

    def forward1(st, step, i):
        return remote(recv1.at[st, step, i], recv1.at[st, step + 1, i], s1.at[st, step + 1, i], r1.at[st, step + 1, i], next_of(st, 0))

    def arrived1(st, step, i):
        return remote(recv1.at[st, step, i], recv1.at[st, step, i], s1.at[st, step, i], r1.at[st, step, i], next_of(st, 0))

    def fetch(st, n):
        return pltpu.make_async_copy(grad_view(g_ref, STREAMS[st], ring, 2 + n // 4, n % 4), local.at[st, n % 2], l_sem.at[st, n % 2])

    def send2(st, step):
        src = recv1.at[st, 2, 0] if step == 0 else recv2.at[st, step - 1]
        return remote(src, recv2.at[st, step], s2.at[st, step], r2.at[st, step], next_of(st, 1))

    def send3(st, step):
        src = recv2.at[st, 2, back_of(st, 2, 1)] if step == 0 else recv3.at[st, step - 1]
        return remote(src, recv3.at[st, step], s3.at[st, step], r3.at[st, step], next_of(st, 2))

    state_in = [pltpu.make_async_copy(src, state.at[j], in_sem.at[j]) for j, src in enumerate((w_ref, m_ref, v_ref))]
    all_st = range(len(STREAMS))
    early, late = all_st[:EARLY], all_st[EARLY:]
    for i in range(4):
        for st in early:
            first_load(st, i).start()
        if i == 0:
            for st in all_st:
                for n in range(2):
                    fetch(st, n).start()
    pl.semaphore_wait(barrier, sum(sizes) - len(sizes))
    for i in range(4):
        for st in late:
            first_send(st, i).start()
    for copy in state_in:
        copy.start()

    def accumulate(st, step, i, more):
        n = step * 4 + i
        if step == 0 and st < EARLY:
            first_load(st, i).wait()
        else:
            arrived1(st, step, i).wait_recv()
        fetch(st, n).wait()
        recv1[st, step, i] = recv1[st, step, i] + local[st, n % 2]
        if more:
            fetch(st, n + 2).start()

    for step in range(2):
        def phase1(i, carry):
            for st in all_st:
                accumulate(st, step, i, True)
                forward1(st, step, i).start()
            return carry

        lax.fori_loop(0, 4, phase1, 0)
    for i in range(4):
        for st in all_st:
            accumulate(st, 2, i, i < 2)
            if i == 0:
                send2(st, 0).start()
        if i > 0:
            for st in all_st:
                send2(st, i - 1).wait_recv()
                recv2[st, i - 1] = recv2[st, i - 1] + recv1[st, 2, i]
                if i < 3:
                    send2(st, i).start()
                else:
                    send3(st, 0).start()
    for step in range(3):
        for st in all_st:
            send3(st, step).wait_recv()
            recv3[st, step] = recv3[st, step] + recv2[st, 2, back_of(st, 2, 2 + step)]
            if step < 2:
                send3(st, step + 1).start()

    for copy in state_in:
        copy.wait()
    total = jnp.zeros(TILE, jnp.float32)
    for st in all_st:
        piece = recv3[st, 2]
        total = total + jnp.sum(piece * piece, axis=0)

    parts = (total, loss_ref[...])
    pending = []
    for phase, size in enumerate(sizes):
        mine = (stage * 4 + coords[2], coords[0] * 4 + coords[1])[phase]
        nbuf[phase, mine, 0], nbuf[phase, mine, 1] = parts
        sends = [remote(nbuf.at[phase, mine], nbuf.at[phase, mine], ns.at[phase, delta], nr.at[phase, delta], friend(phase, delta)) for delta in range(1, size)]
        for send in sends:
            send.start()
        for send in sends:
            send.wait_recv()
        parts = tuple(sum((nbuf[phase, slot, j] for slot in range(1, size)), nbuf[phase, 0, j]) for j in range(2))
        pending += sends

    stat_out[0] = jnp.sum(parts[1])
    norm = jnp.sqrt(jnp.full((8, 128), jnp.sum(parts[0]), jnp.float32))
    clip = jnp.minimum(1.0, tau_clip / norm)

    def update(width):
        def group(k, carry):
            for h in range(2):
                for t in range(PART):
                    rows = pl.ds(k * 192 + (t // width) * (8 * width) + t % width, 8, stride=width)
                    grad = clip * recv3[(1 - h) * EARLY + 2 * k + t // HALF_PART, 2, t % HALF_PART]
                    m_new = BETA_ONE * state[1, h, rows, :] + (1.0 - BETA_ONE) * grad
                    v_new = BETA_TWO * state[2, h, rows, :] + (1.0 - BETA_TWO) * grad * grad
                    m_hat = m_new * (1.0 / (1.0 - BETA_ONE ** ADAM_STEP))
                    v_hat = v_new * (1.0 / (1.0 - BETA_TWO ** ADAM_STEP))
                    w_old = state[0, h, rows, :]
                    w_new = w_old - learn_rate * (m_hat / (jnp.sqrt(v_hat) + ADAM_EPS) + WEIGHT_DECAY * w_old)
                    state[0, h, rows, :] = w_new
                    state[1, h, rows, :] = m_new
                    state[2, h, rows, :] = v_new
                    full_out[(h,) + coords + (k * PART + t,)] = w_new.astype(jnp.bfloat16)
            return carry

        lax.fori_loop(0, 3, group, 0)

    @pl.when(me < 32)
    def _():
        update(24)

    @pl.when(me >= 32)
    def _():
        update(6)

    def full_part(st, on_a, on_b, on_c):
        k, d = streams[st]
        return full_out.at[(d,) + pick(k, on_a, on_b, on_c) + (pl.ds(PART * k, PART),)]

    def along(st, phase):
        k, d = streams[st]
        return peer(ORDERS[k][phase], sgn(d))

    def coord_of(st, phase, delta):
        k, d = streams[st]
        return ring(ORDERS[k][phase], -sgn(d) * delta)

    def gather1(st, step):
        k, d = streams[st]
        place = full_part(st, coord_of(st, 0, 0), coord_of(st, 1, 0), coord_of(st, 2, step))
        return remote(place, place, t1.at[st, step], q1.at[st, step], along(st, 2))

    def gather2(st, step):
        place = full_part(st, coord_of(st, 0, 0), coord_of(st, 1, step), slice(None))
        return remote(place, place, t2.at[st, step], q2.at[st, step], along(st, 1))

    def gather3(st, step, i):
        place = full_part(st, coord_of(st, 0, step), coord_of(st, 1, i), slice(None))
        return remote(place, place, t3.at[st, step, i], q3.at[st, step, i], along(st, 0))

    for st in range(6):
        gather1(st, 0).start()
    for step in range(3):
        for st in range(6):
            gather1(st, step).wait_recv()
            if step < 2:
                gather1(st, step + 1).start()
    for st in range(6):
        gather2(st, 0).start()
        gather3(st, 0, 0).start()
    for step in range(3):
        for st in range(6):
            gather2(st, step).wait_recv()
            if step < 2:
                gather2(st, step + 1).start()
            gather3(st, 0, step + 1).start()

    def phase3(n, carry):
        step, i = n // 4, n % 4
        for st in range(6):
            gather3(st, step, i).wait_recv()
            gather3(st, step + 1, i).start()
        return carry

    lax.fori_loop(0, 8, phase3, 0)
    for i in range(4):
        for st in range(6):
            gather3(st, 2, i).wait_recv()

    def drain(i, carry):
        for step in range(3):
            for st in all_st:
                if step > 0 or st >= EARLY:
                    arrived1(st, step, i).wait_send()
            for st in range(6):
                gather3(st, step, i).wait_send()
        return carry

    lax.fori_loop(0, 4, drain, 0)
    for send in pending:
        send.wait_send()
    for step in range(3):
        for st in all_st:
            send2(st, step).wait_send()
            send3(st, step).wait_send()
        for st in range(6):
            gather1(st, step).wait_send()
            gather2(st, step).wait_send()


def tail(grads, early, w_flat, m_flat, v_flat, loss_tile, tau_clip, learn_rate):
    f32, bf16 = jnp.float32, jnp.bfloat16
    flat = pltpu.VMEM((3,) + w_flat.shape, f32)
    in_vmem = pl.BlockSpec(memory_space=pltpu.VMEM)
    in_any = pl.BlockSpec(memory_space=pl.ANY)
    dma = pltpu.SemaphoreType.DMA
    n_stream = len(STREAMS)
    per_step = (n_stream, 3)
    per_sub = per_step + (4,)
    part = (HALF_PART,) + TILE
    per_place = (6, 3)
    return pl.pallas_call(
        functools.partial(tail_kernel, tau_clip, learn_rate),
        out_shape=(flat, jax.ShapeDtypeStruct((1,), f32), pltpu.VMEM(grads.shape, bf16)),
        in_specs=[in_any] * 5 + [in_vmem],
        out_specs=(in_vmem, pl.BlockSpec(memory_space=pltpu.SMEM), in_vmem),
        scratch_shapes=[
            pltpu.VMEM(per_sub + (4,) + part, f32),
            pltpu.VMEM(per_sub + part, f32),
            pltpu.VMEM(per_step + part, f32),
            pltpu.VMEM((n_stream, 2, 4) + part, f32),
            pltpu.VMEM((2, 16, 2) + TILE, f32),
            *[dma(per_sub)] * 2, *[dma(per_step)] * 4,
            dma((n_stream, 2)), dma((EARLY, 4)), *[dma((2, 16))] * 2, dma((3,)),
            *[dma(per_place)] * 4, *[dma(per_place + (4,))] * 2,
        ],
        compiler_params=pltpu.CompilerParams(collective_id=1, has_side_effects=True, vmem_limit_bytes=VMEM_LIMIT * 7 // 10),
        name="tail",
    )(grads, early, w_flat, m_flat, v_flat, loss_tile)


ROWS = 256
SLOTS = 4
BAND = 256
GELU_K = math.sqrt(2.0 / math.pi)
GELU_C = 0.044715


def gelu_tanh(pre, square):
    return jnp.tanh(pre * (GELU_K + (GELU_K * GELU_C) * square))


def stack_kernel(n_tokens, x_hbm, t_hbm, w1_hbm, w2_hbm, g_out, early_out, loss_out,
                 w1, w2, xs, gs, us, acts, rs, outf, outb, tgt, xt, stage1, stage2,
                 w1_sem, w2_sem, x_sem, t_sem, xsend, xrecv, gsend, grecv, o1_sem, o2_sem, es, er):
    stage, me, coords, ring, peer = torus()
    partner = (1 - stage, me)
    n_half, d_model, d_ff = w1.shape

    def load_w1(h):
        return pltpu.make_async_copy(w1_hbm.at[h], w1.at[h], w1_sem.at[h])

    def load_w2(h):
        return pltpu.make_async_copy(w2_hbm.at[h], w2.at[h], w2_sem.at[h])

    load_x = pltpu.make_async_copy(x_hbm, xs.at[0], x_sem)
    load_t = pltpu.make_async_copy(t_hbm, tgt, t_sem)

    @pl.when(stage == 0)
    def _():
        load_x.start()

    load_w1(0).start()

    barrier = pltpu.get_barrier_semaphore()
    pl.semaphore_signal(barrier, inc=1, device_id=partner, device_id_type=MESH_ID)
    for axis in range(3):
        for d in range(2):
            pl.semaphore_signal(barrier, inc=1, device_id=peer(axis, sgn(d)), device_id_type=MESH_ID)
    pl.semaphore_wait(barrier, 7)

    load_w2(0).start()

    @pl.when(stage == 0)
    def _():
        load_x.wait()

    loss_out[...] = jnp.zeros((8, 128), jnp.float32)

    def dot(lhs, rhs, on_left, on_right):
        return lax.dot_general(lhs, rhs, (((on_left,), (on_right,)), ((), ())), preferred_element_type=jnp.float32)

    def rows_of(c):
        return pl.ds(pl.multiple_of(c * ROWS, ROWS), ROWS)

    def block(i, size):
        return pl.ds(pl.multiple_of(i * size, size), size)

    def send_x(h, c, n):
        cols = block(n, BAND)
        return remote(outf.at[h, c, :, cols], xs.at[h + stage, rows_of(c), cols], xsend.at[h, c, n], xrecv.at[h + stage, c, n], partner)

    def wait_x(h, c, n):
        cols = block(n, BAND)
        remote(outf.at[h, c, :, cols], xs.at[h, rows_of(c), cols], xsend.at[h, c, n], xrecv.at[h, c, n], partner).wait_recv()

    def send_g(h, c, n):
        to, cols = h - 1 + stage, block(n, BAND)
        return remote(outb.at[h, c, :, cols], gs.at[to, rows_of(c), cols], gsend.at[h, c, n], grecv.at[to, c, n], partner)

    def wait_g(h, c, n):
        cols = block(n, BAND)
        remote(outb.at[h, c, :, cols], gs.at[h, rows_of(c), cols], gsend.at[h, c, n], grecv.at[h, c, n], partner).wait_recv()

    def forward(item, carry):
        h, c = item // 2, item % 2
        rows = rows_of(c)

        @pl.when(c == 0)
        def _():
            load_w1(h).wait()

        @pl.when(h + stage > 0)
        def _():
            for n in range(3):
                wait_x(h, c, n)

        def up(f, inner):
            cols = block(f, 512)
            pre = dot(xs[h, rows, :], w1[h, :, cols], 1, 0)
            us[h, rows, cols] = pre
            half = 0.5 * pre
            acts[h, rows, cols] = (half + half * gelu_tanh(pre, pre * pre)).astype(jnp.bfloat16)
            return inner

        lax.fori_loop(0, d_ff // 512, up, 0, unroll=True)

        @pl.when(c == 0)
        def _():
            load_w2(h).wait()

        @pl.when(item == 0)
        def _():
            load_w1(1).start()
            load_w2(1).start()
            load_t.start()

        def down(n, inner):
            cols = block(n, BAND)
            val = dot(acts[h, rows, :], w2[h, :, cols], 1, 0)
            outf[h, c, :, cols] = (xs[h, rows, cols].astype(jnp.float32) + val).astype(jnp.bfloat16)

            @pl.when(h + stage < 2)
            def _():
                send_x(h, c, n).start()

            return inner

        lax.fori_loop(0, d_model // BAND, down, 0)

        @pl.when(h + stage == 2)
        def _():
            @pl.when(c == 0)
            def _():
                load_t.wait()

            residual = outf[h, c].astype(jnp.float32) - tgt[rows, :].astype(jnp.float32)
            gs[h, rows, :] = (residual / n_tokens).astype(jnp.bfloat16)
            square = residual * residual
            part = sum(square[:, 128 * j:128 * (j + 1)] for j in range(d_model // 128))
            loss_out[...] += 0.5 * jnp.sum(part.reshape(ROWS // 8, 8, 128), axis=0)

        return carry

    lax.fori_loop(0, 2 * n_half, forward, 0)

    @pl.when(stage == 0)
    def _():
        load_t.wait()

    def out_one(h, n, i):
        return pltpu.make_async_copy(stage1.at[n % SLOTS, i], g_out.at[h, pl.ds(0, 2), :, :, pl.ds(i * 24 + 2 * n, 2)], o1_sem.at[n % SLOTS, i])

    def out_two(h, m):
        return pltpu.make_async_copy(stage2.at[m % SLOTS], g_out.at[h, 2 + m // 4, m % 4], o2_sem.at[m % SLOTS])

    def early_send(st, i):
        h, k, d = STREAMS[st]
        return remote(grad_view(g_out, STREAMS[st], ring, 1, i), early_out.at[st, i], es.at[st, i], er.at[st, i], peer(ORDERS[k][0], sgn(d)))

    def backward(b, carry):
        h = 1 - b

        def chain(c, inner):
            rows = rows_of(c)

            @pl.when(h + stage < 2)
            def _():
                for n in range(3):
                    wait_g(h, c, n)

            def up(f, deep):
                cols = block(f, 512)
                q = dot(gs[h, rows, :], w2[h, cols, :], 1, 1)
                pre = us[h, rows, cols]
                square = pre * pre
                th = gelu_tanh(pre, square)
                slope = (0.5 + 0.5 * th) + (1.0 - th * th) * (pre * (0.5 * GELU_K + (1.5 * GELU_K * GELU_C) * square))
                rs[rows, cols] = (q * slope).astype(jnp.bfloat16)
                return deep

            lax.fori_loop(0, d_ff // 512, up, 0, unroll=True)

            @pl.when(h + stage > 0)
            def _():
                def down(n, deep):
                    cols = block(n, BAND)
                    val = dot(rs[rows, :], w1[h, cols, :], 1, 1)
                    outb[h, c, :, cols] = (gs[h, rows, cols].astype(jnp.float32) + val).astype(jnp.bfloat16)
                    send_g(h, c, n).start()
                    return deep

                lax.fori_loop(0, d_model // BAND, down, 0)

            return inner

        lax.fori_loop(0, 2, chain, 0)

        xt[...] = xs[h].T

        def grad_one(n, inner):
            @pl.when(n >= SLOTS)
            def _():
                for i in range(3):
                    out_one(h, n, i).wait()

            val = dot(xt[...], rs[:, block(n, BAND)], 1, 0)
            for p in range(32):
                for i in range(3):
                    for j in range(2):
                        stage1[n % SLOTS, i, p // 16, (p // 4) % 4, p % 4, j] = val[p * 24 + i * 8:p * 24 + i * 8 + 8, 128 * j:128 * (j + 1)]
            for i in range(3):
                out_one(h, n, i).start()
            return inner

        lax.fori_loop(0, d_ff // BAND, grad_one, 0)

        def grad_two(m, inner):
            @pl.when(m >= SLOTS)
            def _():
                out_two(h, m).wait()

            val = dot(acts[h, :, block(m, 384)], gs[h], 0, 0)
            for p in range(4):
                for i in range(12):
                    for j in range(6):
                        stage2[m % SLOTS, p, i * 6 + j] = val[p * 96 + i * 8:p * 96 + i * 8 + 8, 128 * j:128 * (j + 1)]
            out_two(h, m).start()
            return inner

        lax.fori_loop(0, d_ff // 384, grad_two, 0)
        for n in range(SLOTS):
            for i in range(3):
                out_one(h, n, i).wait()
            out_two(h, n).wait()

        @pl.when(b == 0)
        def _():
            for i in range(4):
                for st in range(EARLY):
                    early_send(st, i).start()

        return carry

    lax.fori_loop(0, n_half, backward, 0)
    for i in range(4):
        for st in range(EARLY):
            early_send(st, i).wait()

    for h in range(2):
        for c in range(2):
            @pl.when(h + stage < 2)
            def _():
                for n in range(3):
                    send_x(h, c, n).wait_send()

            @pl.when(h + stage > 0)
            def _():
                for n in range(3):
                    send_g(h, c, n).wait_send()


def stack(x_all, t_all, w1, w2, n_tokens):
    rows, d_model = x_all.shape
    d_ff = w1.shape[2]
    bf16, f32 = jnp.bfloat16, jnp.float32
    dma = pltpu.SemaphoreType.DMA
    in_any = pl.BlockSpec(memory_space=pl.ANY)
    return pl.pallas_call(
        functools.partial(stack_kernel, n_tokens),
        out_shape=(jax.ShapeDtypeStruct((2, 4, 4, 4, TILES) + TILE, f32), jax.ShapeDtypeStruct((EARLY, 4, 4, HALF_PART) + TILE, f32), jax.ShapeDtypeStruct(TILE, f32)),
        in_specs=[in_any] * 4,
        out_specs=(in_any, in_any, pl.BlockSpec(memory_space=pltpu.VMEM)),
        scratch_shapes=[
            pltpu.VMEM((2, d_model, d_ff), bf16), pltpu.VMEM((2, d_ff, d_model), bf16),
            pltpu.VMEM((2, rows, d_model), bf16), pltpu.VMEM((2, rows, d_model), bf16),
            pltpu.VMEM((2, rows, d_ff), f32), pltpu.VMEM((2, rows, d_ff), bf16), pltpu.VMEM((rows, d_ff), bf16),
            pltpu.VMEM((2, 2, ROWS, d_model), bf16), pltpu.VMEM((2, 2, ROWS, d_model), bf16), pltpu.VMEM((rows, d_model), bf16), pltpu.VMEM((d_model, rows), bf16),
            pltpu.VMEM((SLOTS, 3, 2, 4, 4, 2) + TILE, f32), pltpu.VMEM((SLOTS, 4, TILES) + TILE, f32),
            dma((2,)), dma((2,)), dma, dma, *[dma((2, 2, 3))] * 4, dma((SLOTS, 3)), dma((SLOTS,)), *[dma((EARLY, 4))] * 2,
        ],
        compiler_params=pltpu.CompilerParams(collective_id=0, has_side_effects=True, vmem_limit_bytes=VMEM_LIMIT),
        name="stack",
    )(x_all, t_all, w1, w2)


def solution(mesh):
    n_stage = mesh.shape["stage"]
    n_data = mesh.shape["data"]

    def device_step(x_loc, t_loc, w1_loc, w2_loc, wm_loc, m_loc, v_loc):
        n_micro, n_tok, d_model = x_loc.shape
        d_ff = w1_loc.shape[4]
        n_tokens = n_micro * n_tok * n_data
        n_blocks = 2 * n_stage
        tau_clip = 0.3 * d_model * math.sqrt(n_blocks * (3.0 / n_tokens + 0.008))
        learn_rate = 0.1 / math.sqrt(4.0 * d_model * n_blocks)
        x_all = x_loc.reshape(n_micro * n_tok, d_model)
        t_all = t_loc.reshape(n_micro * n_tok, d_model)
        grads, early, loss_tile = stack(x_all, t_all, w1_loc[0, :, 0], w2_loc[0, :, 0], n_tokens)
        state, stat, w_full = tail(
            grads, early, wm_loc.reshape(2, 576, 128), m_loc.reshape(2, 576, 128), v_loc.reshape(2, 576, 128),
            loss_tile, tau_clip, learn_rate)
        w1_new = w_full[:, :2].reshape(2, d_model // 8, d_ff // 128, 8, 128).transpose(0, 1, 3, 2, 4).reshape(1, 2, 1, d_model, d_ff)
        w2_new = w_full[:, 2:].reshape(2, d_ff // 8, d_model // 128, 8, 128).transpose(0, 1, 3, 2, 4).reshape(1, 2, 1, d_ff, d_model)
        flat_dims = (1, 2, 1, -1)
        return w1_new, w2_new, *(state[j].reshape(flat_dims) for j in range(3)), stat.reshape(()) / n_tokens

    act_spec = P(None, "data", None)
    flat_spec = P("stage", None, None, "data")
    return jax.shard_map(device_step, mesh=mesh, in_specs=(act_spec, act_spec, P("stage"), P("stage"), flat_spec, flat_spec, flat_spec), out_specs=(P("stage"), P("stage"), flat_spec, flat_spec, flat_spec, P()), check_vma=False)
```
